16 devices in a mesh: dp: 1, sp: 16 (over x, y, z, core).
Axes of the slice: x: 2, y: 2, z: 2, core: 2. Of those that a mesh axis runs over, the one named last changes fastest.
Arguments:
- x: bfloat16 [4096, 2048], P(('dp', 'sp'))
- gain: bfloat16 [2048], replicated
- wq: bfloat16 [2048, 4096], P('sp')
- wk: bfloat16 [2048, 512], P('sp')
- wv: bfloat16 [2048, 512], P('sp')
- wo: bfloat16 [4096, 2048], P('sp')
Outputs:
- output: bfloat16 [4096, 2048], P(('dp', 'sp'))
All inputs are finite; a program needn't handle non-finite values.
Results may differ from the reference program's by a relative error of at most 0.012.
Values are sent between devices in bfloat16 or wider.
A program may use at most 2 GiB of HBM per device.

```python
import jax
import jax.numpy as jnp
from jax import lax

ROWS = 4096
D = 2048
HEADS = 16
KV_HEADS = 2
HEAD = 256
THETA = 10000


def setup_inputs(seed: int = 0, part: int = 0) -> dict:
    kx, kn, kq, kk, kv, ko = jax.random.split(jax.random.key(seed), 6)

    def weights(key, rows, columns):
        return jax.random.normal(key, (rows, columns), jnp.float32) * rows**-0.5

    drawn = {
        "x": jax.random.normal(jax.random.fold_in(kx, part), (ROWS, D), jnp.float32),
        "gain": 1 + 0.1 * jax.random.normal(kn, (D,), jnp.float32),
        "wq": 2 * weights(kq, D, HEADS * HEAD),
        "wk": 2 * weights(kk, D, KV_HEADS * HEAD),
        "wv": 4 * weights(kv, D, KV_HEADS * HEAD),
        "wo": weights(ko, HEADS * HEAD, D),
    }
    return {k: v.astype(jnp.bfloat16) for k, v in drawn.items()}


def normed(x, gain):
    wide = x.astype(jnp.float32)
    scale = lax.rsqrt(jnp.mean(wide * wide, -1, keepdims=True) + 1e-6)
    return (wide * scale * gain.astype(jnp.float32)).astype(jnp.bfloat16)


def turned(t, place, theta):
    half = t.shape[-1] // 2
    angle = place.astype(jnp.float32)[:, None] * theta ** (-jnp.arange(half, dtype=jnp.float32) / half)
    cos, sin = jnp.cos(angle)[:, None], jnp.sin(angle)[:, None]
    a, b = t[..., :half].astype(jnp.float32), t[..., half:].astype(jnp.float32)
    return jnp.concatenate([a * cos - b * sin, b * cos + a * sin], -1).astype(jnp.bfloat16)


def matmul(a, w):
    return jnp.dot(a, w, preferred_element_type=jnp.float32).astype(jnp.bfloat16)


def einsum(form, a, b):
    return jnp.einsum(form, a.astype(jnp.float32), b.astype(jnp.float32))


def attention(q, k, v):
    scores = einsum("tgsd,ugd->gstu", q, k) * q.shape[-1] ** -0.5
    token = jnp.arange(q.shape[0])
    scores = jnp.where(token[:, None] >= token, scores, -jnp.inf)
    weights = jax.nn.softmax(scores, -1).astype(jnp.bfloat16)
    return einsum("gstu,ugd->tgsd", weights, v).astype(jnp.bfloat16)


def reference(x, gain, wq, wk, wv, wo):
    a, place = normed(x, gain), jnp.arange(ROWS)
    q = turned(matmul(a, wq).reshape(ROWS, HEADS, HEAD), place, THETA).reshape(ROWS, KV_HEADS, -1, HEAD)
    k = turned(matmul(a, wk).reshape(ROWS, KV_HEADS, HEAD), place, THETA)
    v = matmul(a, wv).reshape(ROWS, KV_HEADS, HEAD)
    seen = attention(q, k, v).reshape(ROWS, HEADS * HEAD)
    return (x.astype(jnp.float32) + jnp.dot(seen, wo, preferred_element_type=jnp.float32)).astype(jnp.bfloat16)
```

```python
import functools

import jax
import jax.numpy as jnp
from jax import lax
from jax.experimental import pallas as pl
from jax.experimental.pallas import tpu as pltpu
from jax.sharding import PartitionSpec as P

HEAD = 256
THETA = 10000
NEG = -1e30
HIDDEN = 2 * NEG
LOG2E = 1.4426950408889634
MESH = pl.DeviceIdType.MESH
BF16, F32 = jnp.bfloat16, jnp.float32
STRIP = 512
NQ, NO = 4, 8
WKV, WQ, KVL, KVU, WO = 0, 1, 1 + NQ, 2 + NQ, 3 + NQ
PARTS = 3 + NQ + NO
X_WK, X_WV, X_WQ, X_X, X_OUT = 0, 1, 2, 2 + NQ, 3 + NQ
SWAPS = 3 + NQ + NO


def _dot(a, b, ca, cb):
    return lax.dot_general(a, b, (((ca,), (cb,)), ((), ())), preferred_element_type=F32)


def kernel(x_ref, gain_ref, cos_ref, sin_ref, wq_ref, wk_ref, wv_ref, wo_ref, y_ref,
           xs, a_s, wkv_s, wq_s, wo_s, kv_s, q_s, top_s, mix_s, seen_s, part_s, got_s, own_s,
           ss, rs, xss, xrs, ls):
    me = lax.axis_index("sp")
    x, y, z, c = me // 8, (me // 4) % 2, (me // 2) % 2, me % 2
    r = me % 8
    other = 1 - x
    xdev, ydev, zdev, cdev = me + 8 - 16 * x, me + 4 - 8 * y, me + 2 - 4 * z, me + 1 - 2 * c

    def rel(k):
        return 4 * ((y + k // 4) % 2) + 2 * ((z + (k // 2) % 2) % 2) + (c + k % 2) % 2

    first, second = 4 - 2 * c, 2 + 2 * c
    far = me + 2 - 4 * z + c * (4 - 8 * y - 2 + 4 * z)

    def remote(src, dst, ssem, rsem, dev):
        return pltpu.make_async_remote_copy(src_ref=src, dst_ref=dst, send_sem=ssem, recv_sem=rsem,
                                            device_id={"sp": dev}, device_id_type=MESH)

    def hop(at, p, src, slot, dev):
        return remote(at(src), at(src), ss.at[p, slot], rs.at[p, slot], dev)

    def own(at, p):
        hop(at, p, r, 4, ydev).start()
        hop(at, p, r, 2, zdev).start()
        hop(at, p, r, 1, cdev).start()

    def arrived(at, p, slot):
        hop(at, p, rel(slot), slot, cdev).wait_recv()

    def forward(at, p):
        arrived(at, p, first)
        hop(at, p, rel(first), 6, far).start()
        hop(at, p, rel(first), first + 1, cdev).start()
        arrived(at, p, second)
        hop(at, p, rel(second), second + 1, cdev).start()

    def diagonal(at, p):
        arrived(at, p, 6)
        hop(at, p, rel(6), 7, cdev).start()

    def complete(at, p):
        for slot in (1, 3, 5, 7):
            arrived(at, p, slot)

    def sent(at, p):
        for slot in range(1, 8):
            hop(at, p, r, slot, cdev).wait_send()

    wkv_at = lambda s: wkv_s.at[:, s]
    wq_at = lambda j: lambda s: wq_s.at[j, s]
    wo_at = lambda j: lambda s: wo_s.at[j, s]
    kvl_at = lambda s: kv_s.at[s]
    kvu_at = lambda s: kv_s.at[s + 8]

    mine = pl.ds(pl.multiple_of(128 * x, 128), 128)

    def columns(h, width):
        return pl.ds(pl.multiple_of(h, width), width)

    def swap_wk(i, ref):
        return remote(ref.at[:, columns(other * 256, 256)], wkv_s.at[i, r, mine], xss.at[X_WK + i], xrs.at[X_WK + i], xdev)

    def swap_wq(j):
        return remote(wq_ref.at[:, columns(other * 2048 + 512 * j, 512)], wq_s.at[j, r, mine], xss.at[X_WQ + j], xrs.at[X_WQ + j], xdev)

    swap_x = remote(x_ref, xs.at[x], xss.at[X_X], xrs.at[X_X], xdev)

    def swap_out(j):
        return remote(part_s.at[j], got_s.at[j], xss.at[X_OUT + j], xrs.at[X_OUT + j], xdev)

    def local(i, src, dst):
        return pltpu.make_async_copy(src, dst, ls.at[i])

    own_wk = [local(i, ref.at[:, columns(x * 256, 256)], wkv_s.at[i, r, mine]) for i, ref in ((0, wk_ref), (1, wv_ref))]
    own_wq = [local(2 + j, wq_ref.at[:, columns(x * 2048 + 512 * j, 512)], wq_s.at[j, r, mine]) for j in range(NQ)]
    own_x = local(2 + NQ, x_ref, xs.at[x])
    own_wo = [local(3 + NQ + j, wo_ref.at[:, pl.ds(256 * j, 256)], wo_s.at[j, r]) for j in range(NO)]

    def norm(s):
        def rows(i, _):
            at = pl.ds(pl.multiple_of(16 * i, 16), 16)
            wide = xs[s, at, :].astype(F32)
            scale = lax.rsqrt(jnp.mean(wide * wide, -1, keepdims=True) + 1e-6)
            a = (wide * scale * gain_ref[...].astype(F32)).astype(BF16)
            for b in range(16):
                to = 2 * (b % 8) + b // 8
                a_s[s, at, to * 128 : to * 128 + 128] = a[:, b * 128 : b * 128 + 128]

        lax.fori_loop(0, 16, rows, None)

    def turn(t, s):
        t = t.astype(BF16).astype(F32)
        a, b = t[:, :128], t[:, 128:]
        cos, sin = cos_ref[s], sin_ref[s]
        return jnp.concatenate([a * cos - b * sin, b * cos + a * sin], -1).astype(BF16)

    def keys(s):
        a = a_s[s]
        k = _dot(a, wkv_s[0].reshape(2048, 256), 1, 0)
        v = _dot(a, wkv_s[1].reshape(2048, 256), 1, 0)
        kv_s[r + 8 * s, 0] = turn(k, s)
        kv_s[r + 8 * s, 1] = v.astype(BF16).T

    def queries(j):
        w = wq_s[j].reshape(2048, 512)
        for s in range(2):
            t = _dot(a_s[s], w, 1, 0)
            for h in range(2):
                q_s[s, 2 * j + h] = turn(t[:, 256 * h : 256 * h + 256], s)

    e = HEAD**-0.5 * LOG2E

    def unit(i, b, masked):
        k, vt = kv_s[b, 0], jnp.concatenate([kv_s[b, 1], jnp.ones((8, 256), BF16)], axis=0)
        at = [slice(n, n + STRIP) for n in range(0, 2048, STRIP)]
        scores = [_dot(k, q_s[i, 2 * n : 2 * n + 2].reshape(STRIP, 256), 1, 1) for n in range(4)]
        if masked:
            gap = lax.broadcasted_iota(jnp.int32, (256, STRIP), 1) % 256 - lax.broadcasted_iota(jnp.int32, (256, STRIP), 0)
            scores = [jnp.where(gap >= 0, s, HIDDEN) for s in scores]
        weights, keeps = [], []
        for n, s in enumerate(scores):
            old = top_s[i, :, at[n]]
            top = jnp.maximum(old, s.max(axis=0, keepdims=True))
            top_s[i, :, at[n]] = top
            weights.append(jnp.exp2((s - top) * e).astype(BF16))
            keeps.append(jnp.exp2((old - top) * e))
        for n in range(4):
            mix_s[i, :, at[n]] = mix_s[i, :, at[n]] * keeps[n] + _dot(vt, weights[n], 1, 0)

    def step(i):
        b = rel(i)
        units = 1 + 2 * ((r + 8 - b) // 8)
        lax.fori_loop(0, units, lambda u, _: unit((u + 1) % 2, b + 8 * (u // 2), False), None)

    def finish(i, _):
        for h in range(8):
            at = slice(256 * h, 256 * h + 256)
            seen_s[i, :, at] = (mix_s[i, :256, at] * (1 / mix_s[i, 256:257, at])).astype(BF16).T

    def project(j):
        w = wo_s[j].reshape(2048, 256)
        part_s[j] = _dot(seen_s[other], w, 1, 0).astype(BF16)
        own_s[j] = _dot(seen_s[x], w, 1, 0)

    def collect(j):
        swap_out(j).wait_recv()
        at = columns(256 * j, 256)
        y_ref[:, at] = (xs[x, :, at].astype(F32) + own_s[j] + got_s[j].astype(F32)).astype(BF16)

    barrier = pltpu.get_barrier_semaphore()
    for dev in (xdev, ydev, zdev, cdev):
        pl.semaphore_signal(barrier, inc=1, device_id={"sp": dev}, device_id_type=MESH)
    own_x.start()
    for copy in own_wo[:2] + own_wk + own_wq + own_wo[2:]:
        copy.start()
    pl.semaphore_wait(barrier, 4)
    swap_wk(0, wk_ref).start()
    swap_wk(1, wv_ref).start()
    for j in range(NQ):
        swap_wq(j).start()
    swap_x.start()

    for j in (0, 1):
        own_wo[j].wait()
        own(wo_at(j), WO + j)
    own_x.wait()
    norm(x)
    for i, ref in ((0, wk_ref), (1, wv_ref)):
        own_wk[i].wait()
        swap_wk(i, ref).wait_recv()
    own(wkv_at, WKV)
    forward(wo_at(0), WO)
    for j in range(2):
        own_wq[j].wait()
        swap_wq(j).wait_recv()
        own(wq_at(j), WQ + j)
        if j == 0:
            forward(wo_at(1), WO + 1)
    diagonal(wo_at(0), WO)
    forward(wkv_at, WKV)
    diagonal(wo_at(1), WO + 1)
    forward(wq_at(0), WQ)
    own_wq[2].wait()
    swap_wq(2).wait_recv()
    own(wq_at(2), WQ + 2)
    diagonal(wkv_at, WKV)
    forward(wq_at(1), WQ + 1)
    own_wq[3].wait()
    swap_wq(3).wait_recv()
    own(wq_at(3), WQ + 3)
    diagonal(wq_at(0), WQ)
    complete(wkv_at, WKV)
    keys(x)
    swap_x.wait_recv()
    norm(other)
    keys(other)
    forward(wq_at(2), WQ + 2)
    diagonal(wq_at(1), WQ + 1)
    own(kvl_at, KVL)
    own(kvu_at, KVU)

    def ask(j, _):
        @pl.when(j == 1)
        def _():
            forward(wq_at(3), WQ + 3)

        @pl.when(j >= 2)
        def _():
            diagonal(wq_at(j), WQ + j)

        complete(wq_at(j), WQ + j)
        queries(j)

    lax.fori_loop(0, NQ, ask, None)

    top_s[...] = jnp.full(top_s.shape, NEG, F32)
    mix_s[...] = jnp.zeros(mix_s.shape, F32)
    lax.fori_loop(0, 2, lambda i, _: unit(i, r + 8 * i, True), None)
    unit(1, r, False)

    def attend(i, _):
        @pl.when(i == 2)
        def _():
            forward(kvl_at, KVL)
            for j in (2, 3):
                own_wo[j].wait()
                own(wo_at(j), WO + j)
            forward(kvu_at, KVU)

        @pl.when(i == 4)
        def _():
            diagonal(kvl_at, KVL)

        @pl.when(i == 6)
        def _():
            forward(wo_at(2), WO + 2)
            diagonal(kvu_at, KVU)
            own_wo[4].wait()
            own(wo_at(4), WO + 4)

        @pl.when(i == 7)
        def _():
            forward(wo_at(3), WO + 3)
            diagonal(wo_at(2), WO + 2)
            own_wo[5].wait()
            own(wo_at(5), WO + 5)

        @pl.when(i % 2 == 1)
        def _():
            arrived(kvl_at, KVL, i)
            arrived(kvu_at, KVU, i)

        step(i)

    lax.fori_loop(1, 8, attend, None)
    lax.fori_loop(0, 2, finish, None)
    for j in (6, 7):
        own_wo[j].wait()

    def output(j, _):
        @pl.when((j >= 2) & (j < NO - 2))
        def _():
            forward(wo_at(j + 2), WO + j + 2)

        @pl.when((j >= 2) & (j < NO - 1))
        def _():
            diagonal(wo_at(j + 1), WO + j + 1)

        @pl.when((j >= 2) & (j < 4))
        def _():
            own(wo_at(j + 4), WO + j + 4)

        complete(wo_at(j), WO + j)
        project(j)
        swap_out(j).start()

        @pl.when(j > 0)
        def _():
            collect(j - 1)

    lax.fori_loop(0, NO, output, None)
    collect(NO - 1)

    for i, ref in ((0, wk_ref), (1, wv_ref)):
        swap_wk(i, ref).wait_send()
    for j in range(NQ):
        swap_wq(j).wait_send()
    swap_x.wait_send()
    sent(wkv_at, WKV)
    sent(kvl_at, KVL)
    sent(kvu_at, KVU)

    def drain_q(j, _):
        sent(wq_at(j), WQ + j)

    def drain_o(j, _):
        sent(wo_at(j), WO + j)
        swap_out(j).wait_send()

    lax.fori_loop(0, NQ, drain_q, None)
    lax.fori_loop(0, NO, drain_o, None)


def solution(mesh):
    def step(x, gain, wq, wk, wv, wo):
        r = lax.axis_index("sp") % 8
        block = (r + 8 * jnp.arange(2))[:, None]
        place = 256 * block + jnp.arange(256)
        half = HEAD // 2
        angle = place.astype(F32)[..., None] * THETA ** (-jnp.arange(half, dtype=F32) / half)
        anywhere, vmem = pl.BlockSpec(memory_space=pl.ANY), pl.BlockSpec(memory_space=pltpu.VMEM)
        return pl.pallas_call(
            kernel,
            out_shape=jax.ShapeDtypeStruct((256, 2048), BF16),
            in_specs=[anywhere, vmem, vmem, vmem, anywhere, anywhere, anywhere, anywhere],
            out_specs=vmem,
            scratch_shapes=[
                pltpu.VMEM((2, 256, 2048), BF16),
                pltpu.VMEM((2, 256, 2048), BF16),
                pltpu.VMEM((2, 8, 256, 256), BF16),
                pltpu.VMEM((NQ, 8, 256, 512), BF16),
                pltpu.VMEM((NO, 8, 256, 256), BF16),
                pltpu.VMEM((16, 2, 256, 256), BF16),
                pltpu.VMEM((2, 8, 256, 256), BF16),
                pltpu.VMEM((2, 1, 2048), F32),
                pltpu.VMEM((2, 264, 2048), F32),
                pltpu.VMEM((2, 256, 2048), BF16),
                pltpu.VMEM((NO, 256, 256), BF16),
                pltpu.VMEM((NO, 256, 256), BF16),
                pltpu.VMEM((NO, 256, 256), F32),
                pltpu.SemaphoreType.DMA((PARTS, 8)),
                pltpu.SemaphoreType.DMA((PARTS, 8)),
                pltpu.SemaphoreType.DMA((SWAPS,)),
                pltpu.SemaphoreType.DMA((SWAPS,)),
                pltpu.SemaphoreType.DMA((3 + NQ + NO,)),
            ],
            compiler_params=pltpu.CompilerParams(collective_id=0, has_side_effects=True, vmem_limit_bytes=58 * 2**20),
        )(x, gain.reshape(1, 2048), jnp.cos(angle), jnp.sin(angle), wq, wk, wv, wo)

    tokens, whole = P(("dp", "sp"), None), P("sp", None)
    return jax.shard_map(
        step,
        mesh=mesh,
        in_specs=(tokens, P(None), whole, whole, whole, whole),
        out_specs=tokens,
        check_vma=False,
    )
```

```python
import functools

import jax
import jax.numpy as jnp
import numpy as np
from jax import lax
from jax.experimental import pallas as pl
from jax.experimental.pallas import tpu as pltpu
from jax.sharding import PartitionSpec as P

HEAD = 256
THETA = 10000
NEG = -1e30
HIDDEN = 2 * NEG
LOG2E = 1.4426950408889634
MESH = pl.DeviceIdType.MESH
BF16, F32 = jnp.bfloat16, jnp.float32
STRIP = 512
NQ, NO = 4, 8
WKV, WQ, KVO, KVP, WO = 0, 2, 2 + NQ, 3 + NQ, 4 + NQ
PARTS = 4 + NQ + NO


def _dot(a, b, ca, cb):
    return lax.dot_general(a, b, (((ca,), (cb,)), ((), ())), preferred_element_type=F32)


def kernel(x_ref, gain_ref, freq_ref, wq_ref, wk_ref, wv_ref, wo_ref, y_ref,
           xs, a_s, cos_s, sin_s, wkv_s, wq_s, wo_s, kv_s, q_s, top_s, mix_s, seen_s, part_s, got_s, own_s,
           ss, rs, xss, xrs, ls):
    me = lax.axis_index("sp")
    x, y, z, c = me // 8, (me // 4) % 2, (me // 2) % 2, me % 2
    r = me % 8
    other = 1 - x
    xdev, ydev, zdev, cdev = me + 8 - 16 * x, me + 4 - 8 * y, me + 2 - 4 * z, me + 1 - 2 * c

    def rel(k):
        return 4 * ((y + k // 4) % 2) + 2 * ((z + (k // 2) % 2) % 2) + (c + k % 2) % 2

    first, second = 4 - 2 * c, 2 + 2 * c
    far = me + 2 - 4 * z + c * (4 - 8 * y - 2 + 4 * z)

    def remote(src, dst, ssem, rsem, dev):
        return pltpu.make_async_remote_copy(src_ref=src, dst_ref=dst, send_sem=ssem, recv_sem=rsem,
                                            device_id={"sp": dev}, device_id_type=MESH)

    def direct(part, slot):
        return rs.at[4 * part[1] + 4 - slot // 2]

    def passed(part, slot):
        return rs.at[4 * PARTS + 4 * (part[1] - KVO) + slot // 2] if part[2] == 2 else rs.at[4 * part[1]]

    def hop(part, src, sem, dev):
        return remote(part[0](src), part[0](src), ss.at[part[2]], sem, dev)

    def own(part):
        hop(part, r, direct(part, 4), ydev).start()
        hop(part, r, direct(part, 2), zdev).start()
        hop(part, r, passed(part, 1), cdev).start()

    def forward(part):
        hop(part, rel(first), direct(part, first), cdev).wait_recv()
        hop(part, rel(first), direct(part, 6), far).start()
        hop(part, rel(first), passed(part, first + 1), cdev).start()
        hop(part, rel(second), direct(part, second), cdev).wait_recv()
        hop(part, rel(second), passed(part, second + 1), cdev).start()

    def diagonal(part):
        hop(part, rel(6), direct(part, 6), cdev).wait_recv()
        hop(part, rel(6), passed(part, 7), cdev).start()

    def complete(part):
        hop(part, pl.ds(0, 4), passed(part, 1), cdev).wait_recv()

    def arrived(part, slot):
        hop(part, rel(slot), passed(part, slot), cdev).wait_recv()

    mine = pl.ds(pl.multiple_of(128 * x, 128), 128)
    theirs = pl.ds(pl.multiple_of(128 * other, 128), 128)
    wka = (lambda s: wkv_s.at[:, s, mine], WKV, 0)
    wkb = (lambda s: wkv_s.at[:, s, theirs], WKV + 1, 0)
    kvo = (lambda s: kv_s.at[s + 8 * x], KVO, 2)
    kvp = (lambda s: kv_s.at[s + 8 * other], KVP, 2)

    def wq(j):
        return (lambda s: wq_s.at[j, s], WQ + j, 1)

    def wo(j):
        return (lambda s: wo_s.at[j, s], WO + j, 3)

    def columns(h, width):
        return pl.ds(pl.multiple_of(h, width), width)

    def swap_wk(i, ref):
        return remote(ref.at[:, columns(other * 256, 256)], wkv_s.at[i, r, mine], xss.at[0], xrs.at[0], xdev)

    def swap_wq(j):
        return remote(wq_ref.at[:, columns(other * 2048 + 512 * j, 512)], wq_s.at[j, r, mine], xss.at[1], xrs.at[2 + j], xdev)

    swap_x = remote(x_ref, xs.at[x], xss.at[2], xrs.at[1], xdev)

    def swap_out(j):
        return remote(part_s.at[j], got_s.at[j], xss.at[3], xrs.at[2 + NQ + j], xdev)

    all_wk = remote(wkv_s.at[:, r, theirs], wkv_s.at[:, r, theirs], xss.at[0], xrs.at[0], xdev)
    all_wq = remote(wq_s.at[:, r, theirs], wq_s.at[:, r, theirs], xss.at[1], xrs.at[2], xdev)
    all_out = remote(part_s, got_s, xss.at[3], xrs.at[2], xdev)

    def local(i, src, dst):
        return pltpu.make_async_copy(src, dst, ls.at[i])

    own_wk = [local(0, ref.at[:, columns(x * 256, 256)], wkv_s.at[i, r, mine]) for i, ref in ((0, wk_ref), (1, wv_ref))]
    own_wq = [local(1, wq_ref.at[:, columns(x * 2048 + 512 * j, 512)], wq_s.at[j, r, mine]) for j in range(NQ)]
    own_x = local(2, x_ref, xs.at[x])
    own_wo = [local(3 + (j > 0), wo_ref.at[:, pl.ds(256 * j, 256)], wo_s.at[j, r]) for j in range(NO)]
    whole_wk = local(0, wkv_s.at[:, r, mine], wkv_s.at[:, r, mine])
    whole_wq = local(1, wq_s.at[:, r, mine], wq_s.at[:, r, mine])
    rest_wo = local(4, wo_s.at[pl.ds(1, NO - 1), r], wo_s.at[pl.ds(1, NO - 1), r])

    def norm(s):
        def rows(i, _):
            at = pl.ds(pl.multiple_of(16 * i, 16), 16)
            wide = xs[s, at, :].astype(F32)
            scale = lax.rsqrt(jnp.mean(wide * wide, -1, keepdims=True) + 1e-6)
            a = (wide * scale * gain_ref[...].astype(F32).reshape(1, 2048)).astype(BF16)
            for b in range(16):
                to = 2 * (b % 8) + b // 8
                a_s[s, at, to * 128 : to * 128 + 128] = a[:, b * 128 : b * 128 + 128]

        lax.fori_loop(0, 16, rows, None)

    def turn(t, s):
        t = t.astype(BF16).astype(F32)
        a, b = t[:, :128], t[:, 128:]
        cos, sin = cos_s[s], sin_s[s]
        return jnp.concatenate([a * cos - b * sin, b * cos + a * sin], -1).astype(BF16)

    def turns():
        freq = freq_ref[...]

        def rows(i, _):
            s, n = i // 16, i % 16
            at = pl.ds(pl.multiple_of(16 * n, 16), 16)
            place = 256 * (r + 8 * s) + 16 * n + lax.broadcasted_iota(jnp.int32, (16, 128), 0)
            angle = place.astype(F32) * freq
            cos_s[s, at, :] = jnp.cos(angle)
            sin_s[s, at, :] = jnp.sin(angle)

        lax.fori_loop(0, 32, rows, None)

    def keys(s):
        a = a_s[s]
        k = _dot(a, wkv_s[0].reshape(2048, 256), 1, 0)
        v = _dot(a, wkv_s[1].reshape(2048, 256), 1, 0)
        kv_s[r + 8 * s, 0] = turn(k, s)
        kv_s[r + 8 * s, 1] = v.astype(BF16).T

    def queries(j):
        w = wq_s[j].reshape(2048, 512)
        for s in range(2):
            t = _dot(a_s[s], w, 1, 0)
            for h in range(2):
                q_s[s, 2 * j + h] = turn(t[:, 256 * h : 256 * h + 256], s)

    e = HEAD**-0.5 * LOG2E

    def unit(i, b, masked):
        k = kv_s[pl.ds(b, 2), 0].reshape(512, 256)
        ones = jnp.ones((8, 256), BF16)
        vt = jnp.concatenate([jnp.concatenate([kv_s[b + n, 1], ones], axis=0) for n in range(2)], axis=1)
        at = [slice(n, n + STRIP) for n in range(0, 2048, STRIP)]
        scores = [_dot(k, q_s[i, 2 * n : 2 * n + 2].reshape(STRIP, 256), 1, 1) for n in range(4)]
        if masked:
            gap = lax.broadcasted_iota(jnp.int32, (512, STRIP), 1) % 256 - lax.broadcasted_iota(jnp.int32, (512, STRIP), 0)
            scores = [jnp.where(gap >= -256 * c, s, HIDDEN) for s in scores]
        weights, keeps = [], []
        for n, s in enumerate(scores):
            old = top_s[i, :, at[n]]
            top = jnp.maximum(old, s.max(axis=0, keepdims=True))
            top_s[i, :, at[n]] = top
            weights.append(jnp.exp2((s - top) * e).astype(BF16))
            keeps.append(jnp.exp2((old - top) * e))
        for n in range(4):
            mix_s[i, :, at[n]] = mix_s[i, :, at[n]] * keeps[n] + _dot(vt, weights[n], 1, 0)

    def pair(i):
        return 4 * ((y + i // 2) % 2) + 2 * ((z + i % 2) % 2)

    def finish(i, _):
        for h in range(8):
            at = slice(256 * h, 256 * h + 256)
            seen_s[i, :, at] = (mix_s[i, :256, at] * (1 / mix_s[i, 256:257, at])).astype(BF16).T

    def project(j):
        w = wo_s[j].reshape(2048, 256)
        part_s[j] = _dot(seen_s[other], w, 1, 0).astype(BF16)
        own_s[j] = _dot(seen_s[x], w, 1, 0)

    def collect(j):
        swap_out(j).wait_recv()
        at = columns(256 * j, 256)
        y_ref[:, at] = (xs[x, :, at].astype(F32) + own_s[j] + got_s[j].astype(F32)).astype(BF16)

    barrier = pltpu.get_barrier_semaphore()
    for dev in (xdev, ydev, zdev, cdev):
        pl.semaphore_signal(barrier, inc=1, device_id={"sp": dev}, device_id_type=MESH)
    for copy in own_wk + own_wo[:1] + [own_x] + own_wq + own_wo[1:]:
        copy.start()
    pl.semaphore_wait(barrier, 4)
    swap_wk(0, wk_ref).start()
    swap_wk(1, wv_ref).start()
    for j in range(NQ):
        swap_wq(j).start()
    swap_x.start()

    def own_q(j):
        swap_wq(j).wait_recv()
        own(wq(j))

    whole_wk.wait()
    own(wka)
    own_wo[0].wait()
    own(wo(0))
    own_x.wait()
    norm(x)
    forward(wka)
    all_wk.wait_recv()
    own(wkb)
    forward(wo(0))
    whole_wq.wait()
    own_q(0)
    diagonal(wka)
    forward(wkb)
    own_q(1)
    turns()
    diagonal(wo(0))
    forward(wq(0))
    own_q(2)
    diagonal(wkb)
    complete(wka)
    complete(wkb)
    keys(x)
    forward(wq(1))
    own_q(3)
    diagonal(wq(0))
    forward(wq(2))
    diagonal(wq(1))
    swap_x.wait_recv()
    norm(other)
    keys(other)
    forward(wq(3))
    own(kvo)
    own(kvp)
    rest_wo.wait()
    own(wo(1))

    def ask(j, _):
        @pl.when(j >= 2)
        def _():
            diagonal(wq(j))

        complete(wq(j))
        queries(j)

    lax.fori_loop(0, NQ, ask, None)

    top_s[...] = jnp.full(top_s.shape, NEG, F32)
    mix_s[...] = jnp.zeros(mix_s.shape, F32)
    arrived(kvo, 1)
    arrived(kvp, 1)
    lax.fori_loop(0, 2, lambda i, _: unit(i, r - c + 8 * i, True), None)
    forward(kvo)
    own(wo(2))

    def attend(n, _):
        i, u = n // 3, n % 3
        b = pair(i)

        def at(when, *what):
            @pl.when(n == when)
            def _():
                for f, part in what:
                    f(part)

        at(2, (forward, kvp), (own, wo(3)))
        at(4, (forward, wo(1)), (own, wo(4)))
        at(6, (diagonal, kvo))
        at(8, (forward, wo(2)), (own, wo(5)))
        at(9, (diagonal, kvp))
        at(11, (forward, wo(3)), (own, wo(6)))

        @pl.when((u == 0) & (i > 0))
        def _():
            arrived(kvo, 2 * i + 1)
            arrived(kvp, 2 * i + 1)

        @pl.when((u == 0) | ((i > 0) & (b < r - c)))
        def _():
            unit((u + 1) % 2, b + 8 * (u // 2), False)

    lax.fori_loop(0, 12, attend, None)
    diagonal(wo(1))
    lax.fori_loop(0, 2, finish, None)

    def output(j, _):
        @pl.when(j > 1)
        def _():
            diagonal(wo(j))

        complete(wo(j))
        project(j)
        swap_out(j).start()

        @pl.when((j > 0) & (j < 5))
        def _():
            forward(wo(j + 3))

        @pl.when(j == 1)
        def _():
            own(wo(7))

        @pl.when(j > 1)
        def _():
            collect(j - 2)

    lax.fori_loop(0, NO, output, None)
    collect(NO - 2)
    collect(NO - 1)
    all_wk.wait_send()
    all_wq.wait_send()
    swap_x.wait_send()
    all_out.wait_send()
    for kind, what in enumerate((wkv_s.at[:, pl.ds(0, 7)], wq_s.at[:, pl.ds(0, 7)], kv_s.at[pl.ds(0, 14)], wo_s.at[:, pl.ds(0, 7)])):
        remote(what, what, ss.at[kind], rs.at[0], cdev).wait_send()


def solution(mesh):
    def step(x, gain, wq, wk, wv, wo):
        half = HEAD // 2
        freq = np.float32(THETA) ** (-np.arange(half, dtype=np.float32) / np.float32(half))
        anywhere, vmem = pl.BlockSpec(memory_space=pl.ANY), pl.BlockSpec(memory_space=pltpu.VMEM)
        return pl.pallas_call(
            kernel,
            out_shape=pltpu.VMEM((256, 2048), BF16),
            in_specs=[anywhere, vmem, vmem, anywhere, anywhere, anywhere, anywhere],
            out_specs=vmem,
            scratch_shapes=[
                pltpu.VMEM((2, 256, 2048), BF16),
                pltpu.VMEM((2, 256, 2048), BF16),
                pltpu.VMEM((2, 256, 128), F32),
                pltpu.VMEM((2, 256, 128), F32),
                pltpu.VMEM((2, 8, 256, 256), BF16),
                pltpu.VMEM((NQ, 8, 256, 512), BF16),
                pltpu.VMEM((NO, 8, 256, 256), BF16),
                pltpu.VMEM((16, 2, 256, 256), BF16),
                pltpu.VMEM((2, 8, 256, 256), BF16),
                pltpu.VMEM((2, 1, 2048), F32),
                pltpu.VMEM((2, 264, 2048), F32),
                pltpu.VMEM((2, 256, 2048), BF16),
                pltpu.VMEM((NO, 256, 256), BF16),
                pltpu.VMEM((NO, 256, 256), BF16),
                pltpu.VMEM((NO, 256, 256), F32),
                pltpu.SemaphoreType.DMA((4,)),
                pltpu.SemaphoreType.DMA((4 * PARTS + 8,)),
                pltpu.SemaphoreType.DMA((4,)),
                pltpu.SemaphoreType.DMA((2 + NQ + NO,)),
                pltpu.SemaphoreType.DMA((5,)),
            ],
            compiler_params=pltpu.CompilerParams(collective_id=0, has_side_effects=True, vmem_limit_bytes=58 * 2**20),
        )(x, gain, jnp.asarray(freq.astype(np.float32)).reshape(1, half), wq, wk, wv, wo)

    tokens, whole = P(("dp", "sp"), None), P("sp", None)
    return jax.shard_map(
        step,
        mesh=mesh,
        in_specs=(tokens, P(None), whole, whole, whole, whole),
        out_specs=tokens,
        check_vma=False,
    )
```

```python
import functools

import jax
import jax.numpy as jnp
import numpy as np
from jax import lax
from jax.experimental import pallas as pl
from jax.experimental.pallas import tpu as pltpu
from jax.sharding import PartitionSpec as P

HEAD = 256
THETA = 10000
NEG = -1e30
HIDDEN = 2 * NEG
LOG2E = 1.4426950408889634
MESH = pl.DeviceIdType.MESH
BF16, F32 = jnp.bfloat16, jnp.float32
STRIP = 512
NQ, NO = 4, 8
WKV, WQ, KVO, KVP, WO = 0, 2, 2 + NQ, 3 + NQ, 4 + NQ
PARTS = 4 + NQ + NO


def _dot(a, b, ca, cb):
    return lax.dot_general(a, b, (((ca,), (cb,)), ((), ())), preferred_element_type=F32)


def kernel(x_ref, gain_ref, freq_ref, wq_ref, wk_ref, wv_ref, wo_ref, y_ref,
           xs, a_s, cos_s, sin_s, wkv_s, wq_s, wo_s, kv_s, q_s, top_s, mix_s, seen_s, part_s, got_s, own_s,
           ss, rs, xss, xrs, ls):
    me = lax.axis_index("sp")
    x, y, z, c = me // 8, (me // 4) % 2, (me // 2) % 2, me % 2
    r = me % 8
    other = 1 - x
    xdev, ydev, zdev, cdev = me + 8 - 16 * x, me + 4 - 8 * y, me + 2 - 4 * z, me + 1 - 2 * c

    def rel(k):
        return 4 * ((y + k // 4) % 2) + 2 * ((z + (k // 2) % 2) % 2) + (c + k % 2) % 2

    first, second = 4 - 2 * c, 2 + 2 * c
    far = me + 2 - 4 * z + c * (4 - 8 * y - 2 + 4 * z)

    def remote(src, dst, ssem, rsem, dev):
        return pltpu.make_async_remote_copy(src_ref=src, dst_ref=dst, send_sem=ssem, recv_sem=rsem,
                                            device_id={"sp": dev}, device_id_type=MESH)

    def direct(part, slot):
        return rs.at[4 * part[1] + 4 - slot // 2]

    def passed(part, slot):
        return rs.at[4 * PARTS + 4 * (part[1] - KVO) + slot // 2] if part[2] == 2 else rs.at[4 * part[1]]

    def hop(part, src, sem, dev):
        return remote(part[0](src), part[0](src), ss.at[part[2]], sem, dev)

    def own(part):
        hop(part, r, direct(part, 4), ydev).start()
        hop(part, r, direct(part, 2), zdev).start()
        hop(part, r, passed(part, 1), cdev).start()

    def onward(part):
        hop(part, rel(first), direct(part, first), cdev).wait_recv()
        hop(part, rel(first), direct(part, 6), far).start()
        hop(part, rel(first), passed(part, first + 1), cdev).start()

    def across(part):
        hop(part, rel(second), direct(part, second), cdev).wait_recv()
        hop(part, rel(second), passed(part, second + 1), cdev).start()

    def forward(part):
        onward(part)
        across(part)

    def diagonal(part):
        hop(part, rel(6), direct(part, 6), cdev).wait_recv()
        hop(part, rel(6), passed(part, 7), cdev).start()

    def complete(part):
        hop(part, pl.ds(0, 4), passed(part, 1), cdev).wait_recv()

    def arrived(part, slot):
        hop(part, rel(slot), passed(part, slot), cdev).wait_recv()

    mine = pl.ds(pl.multiple_of(128 * x, 128), 128)
    theirs = pl.ds(pl.multiple_of(128 * other, 128), 128)
    wka = (lambda s: wkv_s.at[:, s, mine], WKV, 0)
    wkb = (lambda s: wkv_s.at[:, s, theirs], WKV + 1, 0)
    kvo = (lambda s: kv_s.at[s + 8 * x], KVO, 2)
    kvp = (lambda s: kv_s.at[s + 8 * other], KVP, 2)

    def wq(j):
        return (lambda s: wq_s.at[j, s], WQ + j, 1)

    def wo(j):
        return (lambda s: wo_s.at[j, s], WO + j, 3)

    def columns(h, width):
        return pl.ds(pl.multiple_of(h, width), width)

    def swap_wk(i, ref):
        return remote(ref.at[:, columns(other * 256, 256)], wkv_s.at[i, r, mine], xss.at[0], xrs.at[0], xdev)

    def swap_wq(j):
        return remote(wq_ref.at[:, columns(other * 2048 + 512 * j, 512)], wq_s.at[j, r, mine], xss.at[1], xrs.at[2 + j], xdev)

    swap_x = remote(x_ref, xs.at[x], xss.at[2], xrs.at[1], xdev)

    def swap_out(j):
        return remote(part_s.at[j], got_s.at[j], xss.at[3], xrs.at[2 + NQ + j], xdev)

    all_wk = remote(wkv_s.at[:, r, theirs], wkv_s.at[:, r, theirs], xss.at[0], xrs.at[0], xdev)
    all_wq = remote(wq_s.at[:, r, theirs], wq_s.at[:, r, theirs], xss.at[1], xrs.at[2], xdev)
    all_out = remote(part_s, got_s, xss.at[3], xrs.at[2], xdev)

    def local(i, src, dst):
        return pltpu.make_async_copy(src, dst, ls.at[i])

    own_wk = [local(0, ref.at[:, columns(x * 256, 256)], wkv_s.at[i, r, mine]) for i, ref in ((0, wk_ref), (1, wv_ref))]
    own_wq = [local(1, wq_ref.at[:, columns(x * 2048 + 512 * j, 512)], wq_s.at[j, r, mine]) for j in range(NQ)]
    own_x = local(2, x_ref, xs.at[x])
    own_wo = [local(3 + (j > 0), wo_ref.at[:, pl.ds(256 * j, 256)], wo_s.at[j, r]) for j in range(NO)]
    whole_wk = local(0, wkv_s.at[:, r, mine], wkv_s.at[:, r, mine])
    whole_wq = local(1, wq_s.at[:, r, mine], wq_s.at[:, r, mine])
    rest_wo = local(4, wo_s.at[pl.ds(1, NO - 1), r], wo_s.at[pl.ds(1, NO - 1), r])

    def norm(s):
        def rows(i, _):
            at = pl.ds(pl.multiple_of(16 * i, 16), 16)
            wide = xs[s, at, :].astype(F32)
            scale = lax.rsqrt(jnp.mean(wide * wide, -1, keepdims=True) + 1e-6)
            a = (wide * scale * gain_ref[...].astype(F32).reshape(1, 2048)).astype(BF16)
            for b in range(16):
                to = 2 * (b % 8) + b // 8
                a_s[s, at, to * 128 : to * 128 + 128] = a[:, b * 128 : b * 128 + 128]

        lax.fori_loop(0, 16, rows, None)

    def turn(t, s):
        t = t.astype(BF16).astype(F32)
        a, b = t[:, :128], t[:, 128:]
        cos, sin = cos_s[s], sin_s[s]
        return jnp.concatenate([a * cos - b * sin, b * cos + a * sin], -1).astype(BF16)

    def turns():
        freq = freq_ref[...]

        def rows(i, _):
            s, n = i // 16, i % 16
            at = pl.ds(pl.multiple_of(16 * n, 16), 16)
            place = 256 * (r + 8 * s) + 16 * n + lax.broadcasted_iota(jnp.int32, (16, 128), 0)
            angle = place.astype(F32) * freq
            cos_s[s, at, :] = jnp.cos(angle)
            sin_s[s, at, :] = jnp.sin(angle)

        lax.fori_loop(0, 32, rows, None)

    def keys(s):
        a = a_s[s]
        k = _dot(a, wkv_s[0].reshape(2048, 256), 1, 0)
        v = _dot(a, wkv_s[1].reshape(2048, 256), 1, 0)
        kv_s[r + 8 * s, 0] = turn(k, s)
        kv_s[r + 8 * s, 1] = v.astype(BF16).T

    def queries(j):
        w = wq_s[j].reshape(2048, 512)
        for s in range(2):
            t = _dot(a_s[s], w, 1, 0)
            for h in range(2):
                q_s[s, 2 * j + h] = turn(t[:, 256 * h : 256 * h + 256], s)

    e = HEAD**-0.5 * LOG2E

    def unit(i, b, masked):
        k = kv_s[pl.ds(b, 2), 0].reshape(512, 256)
        ones = jnp.ones((8, 256), BF16)
        vt = jnp.concatenate([jnp.concatenate([kv_s[b + n, 1], ones], axis=0) for n in range(2)], axis=1)
        at = [slice(n, n + STRIP) for n in range(0, 2048, STRIP)]
        scores = [_dot(k, q_s[i, 2 * n : 2 * n + 2].reshape(STRIP, 256), 1, 1) for n in range(4)]
        if masked:
            gap = lax.broadcasted_iota(jnp.int32, (512, STRIP), 1) % 256 - lax.broadcasted_iota(jnp.int32, (512, STRIP), 0)
            scores = [jnp.where(gap >= -256 * c, s, HIDDEN) for s in scores]
        weights, keeps = [], []
        for n, s in enumerate(scores):
            old = top_s[i, :, at[n]]
            top = jnp.maximum(old, s.max(axis=0, keepdims=True))
            top_s[i, :, at[n]] = top
            weights.append(jnp.exp2((s - top) * e).astype(BF16))
            keeps.append(jnp.exp2((old - top) * e))
        for n in range(4):
            mix_s[i, :, at[n]] = mix_s[i, :, at[n]] * keeps[n] + _dot(vt, weights[n], 1, 0)

    def pair(i):
        return 4 * ((y + i // 2) % 2) + 2 * ((z + i % 2) % 2)

    def finish(i):
        for h in range(8):
            at = slice(256 * h, 256 * h + 256)
            seen_s[i, :, at] = (mix_s[i, :256, at] * (1 / mix_s[i, 256:257, at])).astype(BF16).T

    def share(j, s):
        return _dot(seen_s[s], wo_s[j].reshape(2048, 256), 1, 0)

    def project(j):
        w = wo_s[j].reshape(2048, 256)
        part_s[j] = _dot(seen_s[other], w, 1, 0).astype(BF16)
        own_s[j] = _dot(seen_s[x], w, 1, 0)

    def collect(j):
        swap_out(j).wait_recv()
        at = columns(256 * j, 256)
        y_ref[:, at] = (xs[x, :, at].astype(F32) + own_s[j] + got_s[j].astype(F32)).astype(BF16)

    barrier = pltpu.get_barrier_semaphore()
    for dev in (xdev, ydev, zdev, cdev):
        pl.semaphore_signal(barrier, inc=1, device_id={"sp": dev}, device_id_type=MESH)
    for copy in own_wk + own_wo[:1] + [own_x] + own_wq + own_wo[1:]:
        copy.start()
    pl.semaphore_wait(barrier, 4)
    swap_wk(0, wk_ref).start()
    swap_wk(1, wv_ref).start()
    for j in range(NQ):
        swap_wq(j).start()
    swap_x.start()

    def own_q(j):
        swap_wq(j).wait_recv()
        own(wq(j))

    whole_wk.wait()
    own(wka)
    own_wo[0].wait()
    own(wo(0))
    own_x.wait()
    norm(x)
    forward(wka)
    all_wk.wait_recv()
    own(wkb)
    forward(wo(0))
    whole_wq.wait()
    own_q(0)
    diagonal(wka)
    forward(wkb)
    own_q(1)
    turns()
    diagonal(wo(0))
    forward(wq(0))
    own_q(2)
    diagonal(wkb)
    complete(wka)
    complete(wkb)
    keys(x)
    forward(wq(1))
    own_q(3)
    diagonal(wq(0))
    forward(wq(2))
    diagonal(wq(1))
    swap_x.wait_recv()
    norm(other)
    forward(wq(3))
    own(kvo)
    keys(other)
    rest_wo.wait()
    own(kvp)

    def ask(j, _):
        @pl.when(j >= 2)
        def _():
            diagonal(wq(j))

        complete(wq(j))
        queries(j)

    lax.fori_loop(0, NQ, ask, None)

    top_s[...] = jnp.full(top_s.shape, NEG, F32)
    mix_s[...] = jnp.zeros(mix_s.shape, F32)
    onward(kvo)
    arrived(kvo, 1)
    arrived(kvp, 1)
    lax.fori_loop(0, 2, lambda i, _: unit(i, r - c + 8 * i, True), None)
    onward(kvp)
    own(wo(1))
    across(kvo)

    def attend(n, _):
        i = n // 3
        u = lax.select(n < 9, n % 3, (2 * (n - 9) + x) % 3)
        b = pair(i)

        def at(when, *what):
            @pl.when(n == when)
            def _():
                for f, part in what:
                    f(part)

        at(3, (own, wo(2)), (across, kvp))
        at(6, (onward, wo(1)), (own, wo(3)))
        at(7, (diagonal, kvo))
        at(8, (diagonal, kvp), (onward, wo(2)))
        at(9, (own, wo(4)), (across, wo(1)))
        at(10, (onward, wo(3)), (diagonal, wo(1)))
        at(11, (across, wo(2)), (own, wo(5)))

        @pl.when((n % 3 == 0) & (n > 0))
        def _():
            arrived(kvo, 2 * i + 1)
            arrived(kvp, 2 * i + 1)

        @pl.when(n == 11 - x)
        def _():
            finish(other)
            complete(wo(0))
            part_s[0] = share(0, other).astype(BF16)

        @pl.when((u == 0) | ((i > 0) & (b < r - c)))
        def _():
            unit((u + 1) % 2, b + 8 * (u // 2), False)

        @pl.when(n == 11 - x)
        def _():
            swap_out(0).start()

    lax.fori_loop(0, 12, attend, None)
    onward(wo(4))
    diagonal(wo(2))
    across(wo(3))
    finish(x)
    own_s[0] = share(0, x)

    def output(j, _):
        @pl.when(j > 2)
        def _():
            diagonal(wo(j))

        complete(wo(j))
        project(j)
        swap_out(j).start()

        @pl.when(j == 1)
        def _():
            own(wo(6))
            onward(wo(5))

        @pl.when(j == 2)
        def _():
            own(wo(7))
            onward(wo(6))
            across(wo(4))

        @pl.when(j == 3)
        def _():
            across(wo(5))

        @pl.when(j == 4)
        def _():
            onward(wo(7))
            across(wo(6))

        @pl.when(j == 5)
        def _():
            across(wo(7))

        @pl.when(j > 1)
        def _():
            collect(j - 2)

    lax.fori_loop(1, NO, output, None)
    for j in (NO - 2, NO - 1):
        collect(j)
    all_wk.wait_send()
    all_wq.wait_send()
    swap_x.wait_send()
    all_out.wait_send()
    for kind, what in enumerate((wkv_s.at[:, pl.ds(0, 7)], wq_s.at[:, pl.ds(0, 7)], kv_s.at[pl.ds(0, 14)], wo_s.at[:, pl.ds(0, 7)])):
        remote(what, what, ss.at[kind], rs.at[0], cdev).wait_send()


def solution(mesh):
    def step(x, gain, wq, wk, wv, wo):
        half = HEAD // 2
        freq = np.float32(THETA) ** (-np.arange(half, dtype=np.float32) / np.float32(half))
        anywhere, vmem = pl.BlockSpec(memory_space=pl.ANY), pl.BlockSpec(memory_space=pltpu.VMEM)
        return pl.pallas_call(
            kernel,
            out_shape=pltpu.VMEM((256, 2048), BF16),
            in_specs=[anywhere, vmem, vmem, anywhere, anywhere, anywhere, anywhere],
            out_specs=vmem,
            scratch_shapes=[
                pltpu.VMEM((2, 256, 2048), BF16),
                pltpu.VMEM((2, 256, 2048), BF16),
                pltpu.VMEM((2, 256, 128), F32),
                pltpu.VMEM((2, 256, 128), F32),
                pltpu.VMEM((2, 8, 256, 256), BF16),
                pltpu.VMEM((NQ, 8, 256, 512), BF16),
                pltpu.VMEM((NO, 8, 256, 256), BF16),
                pltpu.VMEM((16, 2, 256, 256), BF16),
                pltpu.VMEM((2, 8, 256, 256), BF16),
                pltpu.VMEM((2, 1, 2048), F32),
                pltpu.VMEM((2, 264, 2048), F32),
                pltpu.VMEM((2, 256, 2048), BF16),
                pltpu.VMEM((NO, 256, 256), BF16),
                pltpu.VMEM((NO, 256, 256), BF16),
                pltpu.VMEM((NO, 256, 256), F32),
                pltpu.SemaphoreType.DMA((4,)),
                pltpu.SemaphoreType.DMA((4 * PARTS + 8,)),
                pltpu.SemaphoreType.DMA((4,)),
                pltpu.SemaphoreType.DMA((2 + NQ + NO,)),
                pltpu.SemaphoreType.DMA((5,)),
            ],
            compiler_params=pltpu.CompilerParams(collective_id=0, has_side_effects=True, vmem_limit_bytes=58 * 2**20),
        )(x, gain, jnp.asarray(freq.astype(np.float32)).reshape(1, half), wq, wk, wv, wo)

    tokens, whole = P(("dp", "sp"), None), P("sp", None)
    return jax.shard_map(
        step,
        mesh=mesh,
        in_specs=(tokens, P(None), whole, whole, whole, whole),
        out_specs=tokens,
        check_vma=False,
    )
```

```python
import functools

import jax
import jax.numpy as jnp
import numpy as np
from jax import lax
from jax.experimental import pallas as pl
from jax.experimental.pallas import tpu as pltpu
from jax.sharding import PartitionSpec as P

HEAD = 256
THETA = 10000
NEG = -1e30
HIDDEN = 2 * NEG
LOG2E = 1.4426950408889634
MESH = pl.DeviceIdType.MESH
BF16, F32 = jnp.bfloat16, jnp.float32
STRIP = 512
NQ, NO = 4, 8
WKV, WQ, KVO, KVP, WO = 0, 2, 2 + NQ, 3 + NQ, 4 + NQ
PARTS = 4 + NQ + NO


def _dot(a, b, ca, cb):
    return lax.dot_general(a, b, (((ca,), (cb,)), ((), ())), preferred_element_type=F32)


def kernel(x_ref, gain_ref, freq_ref, wq_ref, wk_ref, wv_ref, wo_ref, y_ref,
           xs, a_s, cos_s, sin_s, wkv_s, wq_s, wo_s, kv_s, q_s, top_s, mix_s, seen_s, part_s, got_s, own_s,
           ss, rs, xss, xrs, ls):
    me = lax.axis_index("sp")
    x, y, z, c = me // 8, (me // 4) % 2, (me // 2) % 2, me % 2
    r = me % 8
    other = 1 - x
    xdev, ydev, zdev, cdev = me + 8 - 16 * x, me + 4 - 8 * y, me + 2 - 4 * z, me + 1 - 2 * c

    def rel(k):
        return 4 * ((y + k // 4) % 2) + 2 * ((z + (k // 2) % 2) % 2) + (c + k % 2) % 2

    first, second = 4 - 2 * c, 2 + 2 * c
    far = me + 2 - 4 * z + c * (4 - 8 * y - 2 + 4 * z)

    def remote(src, dst, ssem, rsem, dev):
        return pltpu.make_async_remote_copy(src_ref=src, dst_ref=dst, send_sem=ssem, recv_sem=rsem,
                                            device_id={"sp": dev}, device_id_type=MESH)

    def direct(part, slot):
        return rs.at[4 * part[1] + 4 - slot // 2]

    def passed(part, slot):
        return rs.at[4 * PARTS + 4 * (part[1] - KVO) + slot // 2] if part[2] == 2 else rs.at[4 * part[1]]

    def hop(part, src, sem, dev):
        return remote(part[0](src), part[0](src), ss.at[part[2]], sem, dev)

    def upward(part, need):
        return pl.when((part[3] == 0) | need) if part[2] == 2 else lambda f: f()

    early, late = c == 0, c == 1
    from_first = (early & (y == 1)) | (late & ((z == 1) | (y == 0)))
    to_core = (early & (y == 1)) | (late & (z == 1))
    from_second = (early & (z == 1)) | (late & (y == 1))
    to_far = (early & (y == 1)) | (late & (y == 0))
    to_y, to_z = y == 0, (z == 0) | (late & (y == 0))

    def own(part):
        @upward(part, to_y)
        def _():
            hop(part, r, direct(part, 4), ydev).start()

        @upward(part, to_z)
        def _():
            hop(part, r, direct(part, 2), zdev).start()

        hop(part, r, passed(part, 1), cdev).start()

    def onward(part):
        @upward(part, from_first)
        def _():
            hop(part, rel(first), direct(part, first), cdev).wait_recv()

        @upward(part, to_far)
        def _():
            hop(part, rel(first), direct(part, 6), far).start()

        @upward(part, to_core)
        def _():
            hop(part, rel(first), passed(part, first + 1), cdev).start()

    def across(part):
        @upward(part, from_second)
        def _():
            hop(part, rel(second), direct(part, second), cdev).wait_recv()
            hop(part, rel(second), passed(part, second + 1), cdev).start()

    def forward(part):
        onward(part)
        across(part)

    def diagonal(part):
        @upward(part, y == 1)
        def _():
            hop(part, rel(6), direct(part, 6), cdev).wait_recv()
            hop(part, rel(6), passed(part, 7), cdev).start()

    def complete(part):
        hop(part, pl.ds(0, 4), passed(part, 1), cdev).wait_recv()

    def arrived(part, slot):
        @upward(part, (slot == 1) | ((slot == 3) & (z == 1)) | ((slot > 3) & (y == 1)))
        def _():
            hop(part, rel(slot), passed(part, slot), cdev).wait_recv()

    mine = pl.ds(pl.multiple_of(128 * x, 128), 128)
    theirs = pl.ds(pl.multiple_of(128 * other, 128), 128)
    wka = (lambda s: wkv_s.at[:, s, mine], WKV, 0)
    wkb = (lambda s: wkv_s.at[:, s, theirs], WKV + 1, 0)
    kvo = (lambda s: kv_s.at[s + 8 * x], KVO, 2, x)
    kvp = (lambda s: kv_s.at[s + 8 * other], KVP, 2, other)

    def wq(j):
        return (lambda s: wq_s.at[j, s], WQ + j, 1)

    def wo(j):
        return (lambda s: wo_s.at[j, s], WO + j, 3)

    def columns(h, width):
        return pl.ds(pl.multiple_of(h, width), width)

    def swap_wk(i, ref):
        return remote(ref.at[:, columns(other * 256, 256)], wkv_s.at[i, r, mine], xss.at[0], xrs.at[0], xdev)

    def swap_wq(j):
        return remote(wq_ref.at[:, columns(other * 2048 + 512 * j, 512)], wq_s.at[j, r, mine], xss.at[1], xrs.at[2 + j], xdev)

    swap_x = remote(x_ref, xs.at[x], xss.at[2], xrs.at[1], xdev)

    def swap_out(j):
        return remote(part_s.at[j], got_s.at[j], xss.at[3], xrs.at[2 + NQ + j], xdev)

    all_wk = remote(wkv_s.at[:, r, theirs], wkv_s.at[:, r, theirs], xss.at[0], xrs.at[0], xdev)
    all_wq = remote(wq_s.at[:, r, theirs], wq_s.at[:, r, theirs], xss.at[1], xrs.at[2], xdev)
    all_out = remote(part_s, got_s, xss.at[3], xrs.at[2], xdev)

    def local(i, src, dst):
        return pltpu.make_async_copy(src, dst, ls.at[i])

    own_wk = [local(0, ref.at[:, columns(x * 256, 256)], wkv_s.at[i, r, mine]) for i, ref in ((0, wk_ref), (1, wv_ref))]
    own_wq = [local(1, wq_ref.at[:, columns(x * 2048 + 512 * j, 512)], wq_s.at[j, r, mine]) for j in range(NQ)]
    own_x = local(2, x_ref, xs.at[x])
    own_wo = [local(3 + (j > 0), wo_ref.at[:, pl.ds(256 * j, 256)], wo_s.at[j, r]) for j in range(NO)]
    whole_wk = local(0, wkv_s.at[:, r, mine], wkv_s.at[:, r, mine])
    whole_wq = local(1, wq_s.at[:, r, mine], wq_s.at[:, r, mine])
    rest_wo = local(4, wo_s.at[pl.ds(1, NO - 1), r], wo_s.at[pl.ds(1, NO - 1), r])

    def norm(s):
        def rows(i, _):
            at = pl.ds(pl.multiple_of(16 * i, 16), 16)
            wide = xs[s, at, :].astype(F32)
            scale = lax.rsqrt(jnp.mean(wide * wide, -1, keepdims=True) + 1e-6)
            a = (wide * scale * gain_ref[...].astype(F32).reshape(1, 2048)).astype(BF16)
            for b in range(16):
                to = 2 * (b % 8) + b // 8
                a_s[s, at, to * 128 : to * 128 + 128] = a[:, b * 128 : b * 128 + 128]

        lax.fori_loop(0, 16, rows, None)

    def turn(t, s):
        t = t.astype(BF16).astype(F32)
        a, b = t[:, :128], t[:, 128:]
        cos, sin = cos_s[s], sin_s[s]
        return jnp.concatenate([a * cos - b * sin, b * cos + a * sin], -1).astype(BF16)

    def turns():
        freq = freq_ref[...]

        def rows(i, _):
            s, n = i // 16, i % 16
            at = pl.ds(pl.multiple_of(16 * n, 16), 16)
            place = 256 * (r + 8 * s) + 16 * n + lax.broadcasted_iota(jnp.int32, (16, 128), 0)
            angle = place.astype(F32) * freq
            cos_s[s, at, :] = jnp.cos(angle)
            sin_s[s, at, :] = jnp.sin(angle)

        lax.fori_loop(0, 32, rows, None)

    def keys(s):
        a = a_s[s]
        k = _dot(a, wkv_s[0].reshape(2048, 256), 1, 0)
        v = _dot(a, wkv_s[1].reshape(2048, 256), 1, 0)
        kv_s[r + 8 * s, 0] = turn(k, s)
        kv_s[r + 8 * s, 1] = v.astype(BF16).T

    def queries(j):
        w = wq_s[j].reshape(2048, 512)
        for s in range(2):
            t = _dot(a_s[s], w, 1, 0)
            for h in range(2):
                q_s[s, 2 * j + h] = turn(t[:, 256 * h : 256 * h + 256], s)

    e = HEAD**-0.5 * LOG2E

    def unit(i, b, masked):
        k = kv_s[pl.ds(b, 2), 0].reshape(512, 256)
        ones = jnp.ones((8, 256), BF16)
        vt = jnp.concatenate([jnp.concatenate([kv_s[b + n, 1], ones], axis=0) for n in range(2)], axis=1)
        at = [slice(n, n + STRIP) for n in range(0, 2048, STRIP)]
        scores = [_dot(k, q_s[i, 2 * n : 2 * n + 2].reshape(STRIP, 256), 1, 1) for n in range(4)]
        if masked:
            gap = lax.broadcasted_iota(jnp.int32, (512, STRIP), 1) % 256 - lax.broadcasted_iota(jnp.int32, (512, STRIP), 0)
            scores = [jnp.where(gap >= -256 * c, s, HIDDEN) for s in scores]
        weights, keeps = [], []
        for n, s in enumerate(scores):
            old = top_s[i, :, at[n]]
            top = jnp.maximum(old, s.max(axis=0, keepdims=True))
            top_s[i, :, at[n]] = top
            weights.append(jnp.exp2((s - top) * e).astype(BF16))
            keeps.append(jnp.exp2((old - top) * e))
        for n in range(4):
            mix_s[i, :, at[n]] = mix_s[i, :, at[n]] * keeps[n] + _dot(vt, weights[n], 1, 0)

    def pair(i):
        return 4 * ((y + i // 2) % 2) + 2 * ((z + i % 2) % 2)

    def finish(i):
        for h in range(8):
            at = slice(256 * h, 256 * h + 256)
            seen_s[i, :, at] = (mix_s[i, :256, at] * (1 / mix_s[i, 256:257, at])).astype(BF16).T

    def share(j, s):
        return _dot(seen_s[s], wo_s[j].reshape(2048, 256), 1, 0)

    def project(j):
        w = wo_s[j].reshape(2048, 256)
        part_s[j] = _dot(seen_s[other], w, 1, 0).astype(BF16)
        own_s[j] = _dot(seen_s[x], w, 1, 0)

    def collect(j):
        swap_out(j).wait_recv()
        at = columns(256 * j, 256)
        y_ref[:, at] = (xs[x, :, at].astype(F32) + own_s[j] + got_s[j].astype(F32)).astype(BF16)

    barrier = pltpu.get_barrier_semaphore()
    for dev in (xdev, ydev, zdev, cdev):
        pl.semaphore_signal(barrier, inc=1, device_id={"sp": dev}, device_id_type=MESH)
    for copy in own_wk + own_wo[:1] + [own_x] + own_wq + own_wo[1:]:
        copy.start()
    pl.semaphore_wait(barrier, 4)
    swap_wk(0, wk_ref).start()
    swap_wk(1, wv_ref).start()
    for j in range(NQ):
        swap_wq(j).start()
    swap_x.start()

    def own_q(j):
        swap_wq(j).wait_recv()
        own(wq(j))

    whole_wk.wait()
    own(wka)
    own_wo[0].wait()
    own(wo(0))
    own_x.wait()
    norm(x)
    forward(wka)
    all_wk.wait_recv()
    own(wkb)
    forward(wo(0))
    whole_wq.wait()
    own_q(0)
    diagonal(wka)
    forward(wkb)
    own_q(1)
    turns()
    diagonal(wo(0))
    forward(wq(0))
    own_q(2)
    diagonal(wkb)
    complete(wka)
    complete(wkb)
    keys(x)
    forward(wq(1))
    own_q(3)
    diagonal(wq(0))
    forward(wq(2))
    diagonal(wq(1))
    swap_x.wait_recv()
    norm(other)
    forward(wq(3))
    own(kvo)
    keys(other)
    rest_wo.wait()
    own(kvp)

    def ask(j, _):
        @pl.when(j >= 2)
        def _():
            diagonal(wq(j))

        complete(wq(j))
        queries(j)

    lax.fori_loop(0, NQ, ask, None)

    top_s[...] = jnp.full(top_s.shape, NEG, F32)
    mix_s[...] = jnp.zeros(mix_s.shape, F32)
    onward(kvo)
    arrived(kvo, 1)
    arrived(kvp, 1)
    lax.fori_loop(0, 2, lambda i, _: unit(i, r - c + 8 * i, True), None)
    onward(kvp)
    own(wo(1))
    across(kvo)

    def attend(n, _):
        i = n // 3
        u = lax.select(n < 9, n % 3, (2 * (n - 9) + x) % 3)
        b = pair(i)

        def at(when, *what):
            @pl.when(n == when)
            def _():
                for f, part in what:
                    f(part)

        at(3, (own, wo(2)), (across, kvp))
        at(6, (onward, wo(1)), (own, wo(3)))
        at(7, (diagonal, kvo))
        at(8, (diagonal, kvp), (onward, wo(2)))
        at(9, (own, wo(4)), (across, wo(1)))
        at(10, (onward, wo(3)), (diagonal, wo(1)))
        at(11, (across, wo(2)), (own, wo(5)))

        @pl.when((n % 3 == 0) & (n > 0))
        def _():
            arrived(kvo, 2 * i + 1)
            arrived(kvp, 2 * i + 1)

        @pl.when(n == 11 - x)
        def _():
            finish(other)
            complete(wo(0))
            part_s[0] = share(0, other).astype(BF16)

        @pl.when((u == 0) | ((i > 0) & (b < r - c)))
        def _():
            unit((u + 1) % 2, b + 8 * (u // 2), False)

        @pl.when(n == 11 - x)
        def _():
            swap_out(0).start()

    lax.fori_loop(0, 12, attend, None)
    onward(wo(4))
    diagonal(wo(2))
    across(wo(3))
    finish(x)
    own_s[0] = share(0, x)

    def output(j, _):
        @pl.when(j > 2)
        def _():
            diagonal(wo(j))

        complete(wo(j))
        project(j)
        swap_out(j).start()

        @pl.when(j == 1)
        def _():
            own(wo(6))
            onward(wo(5))

        @pl.when(j == 2)
        def _():
            own(wo(7))
            onward(wo(6))
            across(wo(4))

        @pl.when(j == 3)
        def _():
            across(wo(5))

        @pl.when(j == 4)
        def _():
            onward(wo(7))
            across(wo(6))

        @pl.when(j == 5)
        def _():
            across(wo(7))

        @pl.when(j > 2)
        def _():
            collect(j - 3)

    lax.fori_loop(1, NO, output, None)
    for j in (NO - 3, NO - 2, NO - 1):
        collect(j)
    all_wk.wait_send()
    all_wq.wait_send()
    swap_x.wait_send()
    all_out.wait_send()
    for kind, what in ((0, wkv_s.at[:, pl.ds(0, 7)]), (1, wq_s.at[:, pl.ds(0, 7)]), (2, kv_s.at[pl.ds(0, 8)]), (3, wo_s.at[:, pl.ds(0, 7)])):
        remote(what, what, ss.at[kind], rs.at[0], cdev).wait_send()
    more = sum(flag.astype(jnp.int32) for flag in (to_y, to_z, to_far, to_core, from_second, y == 1))
    lax.fori_loop(0, more, lambda i, _: remote(kv_s.at[0], kv_s.at[0], ss.at[2], rs.at[0], cdev).wait_send(), None)


def solution(mesh):
    def step(x, gain, wq, wk, wv, wo):
        half = HEAD // 2
        freq = np.float32(THETA) ** (-np.arange(half, dtype=np.float32) / np.float32(half))
        anywhere, vmem = pl.BlockSpec(memory_space=pl.ANY), pl.BlockSpec(memory_space=pltpu.VMEM)
        return pl.pallas_call(
            kernel,
            out_shape=pltpu.VMEM((256, 2048), BF16),
            in_specs=[anywhere, vmem, vmem, anywhere, anywhere, anywhere, anywhere],
            out_specs=vmem,
            scratch_shapes=[
                pltpu.VMEM((2, 256, 2048), BF16),
                pltpu.VMEM((2, 256, 2048), BF16),
                pltpu.VMEM((2, 256, 128), F32),
                pltpu.VMEM((2, 256, 128), F32),
                pltpu.VMEM((2, 8, 256, 256), BF16),
                pltpu.VMEM((NQ, 8, 256, 512), BF16),
                pltpu.VMEM((NO, 8, 256, 256), BF16),
                pltpu.VMEM((16, 2, 256, 256), BF16),
                pltpu.VMEM((2, 8, 256, 256), BF16),
                pltpu.VMEM((2, 1, 2048), F32),
                pltpu.VMEM((2, 264, 2048), F32),
                pltpu.VMEM((2, 256, 2048), BF16),
                pltpu.VMEM((NO, 256, 256), BF16),
                pltpu.VMEM((NO, 256, 256), BF16),
                pltpu.VMEM((NO, 256, 256), F32),
                pltpu.SemaphoreType.DMA((4,)),
                pltpu.SemaphoreType.DMA((4 * PARTS + 8,)),
                pltpu.SemaphoreType.DMA((4,)),
                pltpu.SemaphoreType.DMA((2 + NQ + NO,)),
                pltpu.SemaphoreType.DMA((5,)),
            ],
            compiler_params=pltpu.CompilerParams(collective_id=0, has_side_effects=True, vmem_limit_bytes=58 * 2**20),
        )(x, gain, jnp.asarray(freq.astype(np.float32)).reshape(1, half), wq, wk, wv, wo)

    tokens, whole = P(("dp", "sp"), None), P("sp", None)
    return jax.shard_map(
        step,
        mesh=mesh,
        in_specs=(tokens, P(None), whole, whole, whole, whole),
        out_specs=tokens,
        check_vma=False,
    )
```

```python
import functools

import jax
import jax.numpy as jnp
import numpy as np
from jax import lax
from jax.experimental import pallas as pl
from jax.experimental.pallas import tpu as pltpu
from jax.sharding import PartitionSpec as P

HEAD = 256
THETA = 10000
NEG = -1e30
HIDDEN = 2 * NEG
LOG2E = 1.4426950408889634
MESH = pl.DeviceIdType.MESH
BF16, F32 = jnp.bfloat16, jnp.float32
STRIP = 512
NQ, NO = 4, 8
WKV, WQ, KVO, KVP, WO = 0, 2, 2 + NQ, 3 + NQ, 4 + NQ
PARTS = 4 + NQ + NO


def _dot(a, b, ca, cb):
    return lax.dot_general(a, b, (((ca,), (cb,)), ((), ())), preferred_element_type=F32)


def kernel(x_ref, gain_ref, freq_ref, wq_ref, wk_ref, wv_ref, wo_ref, y_ref,
           xs, a_s, cos_s, sin_s, wkv_s, wq_s, wo_s, kv_s, q_s, top_s, mix_s, seen_s, part_s, got_s, own_s,
           ss, rs, xss, xrs, ls):
    me = lax.axis_index("sp")
    x, y, z, c = me // 8, (me // 4) % 2, (me // 2) % 2, me % 2
    r = me % 8
    other = 1 - x
    xdev, ydev, zdev, cdev = me + 8 - 16 * x, me + 4 - 8 * y, me + 2 - 4 * z, me + 1 - 2 * c

    def rel(k):
        return 4 * ((y + k // 4) % 2) + 2 * ((z + (k // 2) % 2) % 2) + (c + k % 2) % 2

    first, second = 4 - 2 * c, 2 + 2 * c
    far = me + 2 - 4 * z + c * (4 - 8 * y - 2 + 4 * z)

    def remote(src, dst, ssem, rsem, dev):
        return pltpu.make_async_remote_copy(src_ref=src, dst_ref=dst, send_sem=ssem, recv_sem=rsem,
                                            device_id={"sp": dev}, device_id_type=MESH)

    def direct(part, slot):
        return rs.at[4 * part[1] + 4 - slot // 2]

    def passed(part, slot):
        return rs.at[4 * PARTS + 4 * (part[1] - KVO) + slot // 2] if part[2] == 2 else rs.at[4 * part[1]]

    def hop(part, src, sem, dev):
        return remote(part[0](src), part[0](src), ss.at[part[2]], sem, dev)

    def upward(part, need):
        return pl.when((part[3] == 0) | need) if part[2] == 2 else lambda f: f()

    early, late = c == 0, c == 1
    from_first = (early & (y == 1)) | (late & ((z == 1) | (y == 0)))
    to_core = (early & (y == 1)) | (late & (z == 1))
    from_second = (early & (z == 1)) | (late & (y == 1))
    to_far = (early & (y == 1)) | (late & (y == 0))
    to_y, to_z = y == 0, (z == 0) | (late & (y == 0))

    def own(part):
        @upward(part, to_y)
        def _():
            hop(part, r, direct(part, 4), ydev).start()

        @upward(part, to_z)
        def _():
            hop(part, r, direct(part, 2), zdev).start()

        hop(part, r, passed(part, 1), cdev).start()

    def onward(part):
        @upward(part, from_first)
        def _():
            hop(part, rel(first), direct(part, first), cdev).wait_recv()

        @upward(part, to_far)
        def _():
            hop(part, rel(first), direct(part, 6), far).start()

        @upward(part, to_core)
        def _():
            hop(part, rel(first), passed(part, first + 1), cdev).start()

    def across(part):
        @upward(part, from_second)
        def _():
            hop(part, rel(second), direct(part, second), cdev).wait_recv()
            hop(part, rel(second), passed(part, second + 1), cdev).start()

    def forward(part):
        onward(part)
        across(part)

    def diagonal(part):
        @upward(part, y == 1)
        def _():
            hop(part, rel(6), direct(part, 6), cdev).wait_recv()
            hop(part, rel(6), passed(part, 7), cdev).start()

    def complete(part):
        hop(part, pl.ds(0, 4), passed(part, 1), cdev).wait_recv()

    def arrived(part, slot):
        @upward(part, (slot == 1) | ((slot == 3) & (z == 1)) | ((slot > 3) & (y == 1)))
        def _():
            hop(part, rel(slot), passed(part, slot), cdev).wait_recv()

    mine = pl.ds(pl.multiple_of(128 * x, 128), 128)
    theirs = pl.ds(pl.multiple_of(128 * other, 128), 128)
    wka = (lambda s: wkv_s.at[:, s, mine], WKV, 0)
    wkb = (lambda s: wkv_s.at[:, s, theirs], WKV + 1, 0)
    kvo = (lambda s: kv_s.at[s + 8 * x], KVO, 2, x)
    kvp = (lambda s: kv_s.at[s + 8 * other], KVP, 2, other)

    def wq(j):
        return (lambda s: wq_s.at[j, s], WQ + j, 1)

    def wo(j):
        return (lambda s: wo_s.at[j, s], WO + j, 3)

    def columns(h, width):
        return pl.ds(pl.multiple_of(h, width), width)

    def swap_wk(i, ref):
        return remote(ref.at[:, columns(other * 256, 256)], wkv_s.at[i, r, mine], xss.at[0], xrs.at[0], xdev)

    def swap_wq(j):
        return remote(wq_ref.at[:, columns(other * 2048 + 512 * j, 512)], wq_s.at[j, r, mine], xss.at[1], xrs.at[2 + j], xdev)

    swap_x = remote(x_ref, xs.at[x], xss.at[2], xrs.at[1], xdev)

    def swap_out(j):
        return remote(part_s.at[j], got_s.at[j], xss.at[3], xrs.at[2 + NQ + j], xdev)

    all_wk = remote(wkv_s.at[:, r, theirs], wkv_s.at[:, r, theirs], xss.at[0], xrs.at[0], xdev)
    all_wq = remote(wq_s.at[:, r, theirs], wq_s.at[:, r, theirs], xss.at[1], xrs.at[2], xdev)
    all_out = remote(part_s, got_s, xss.at[3], xrs.at[2], xdev)

    def local(i, src, dst):
        return pltpu.make_async_copy(src, dst, ls.at[i])

    own_wk = [local(0, ref.at[:, columns(x * 256, 256)], wkv_s.at[i, r, mine]) for i, ref in ((0, wk_ref), (1, wv_ref))]
    own_wq = [local(1, wq_ref.at[:, columns(x * 2048 + 512 * j, 512)], wq_s.at[j, r, mine]) for j in range(NQ)]
    own_x = local(2, x_ref, xs.at[x])
    own_wo = [local(3 + (j > 0), wo_ref.at[:, pl.ds(256 * j, 256)], wo_s.at[j, r]) for j in range(NO)]
    whole_wk = local(0, wkv_s.at[:, r, mine], wkv_s.at[:, r, mine])
    whole_wq = local(1, wq_s.at[:, r, mine], wq_s.at[:, r, mine])
    rest_wo = local(4, wo_s.at[pl.ds(1, NO - 1), r], wo_s.at[pl.ds(1, NO - 1), r])

    def norm(s):
        def rows(i, _):
            at = pl.ds(pl.multiple_of(16 * i, 16), 16)
            wide = xs[s, at, :].astype(F32)
            scale = lax.rsqrt(jnp.mean(wide * wide, -1, keepdims=True) + 1e-6)
            a = (wide * scale * gain_ref[...].astype(F32).reshape(1, 2048)).astype(BF16)
            for b in range(16):
                to = 2 * (b % 8) + b // 8
                a_s[s, at, to * 128 : to * 128 + 128] = a[:, b * 128 : b * 128 + 128]

        lax.fori_loop(0, 16, rows, None)

    def turn(t, s):
        t = t.astype(BF16).astype(F32)
        a, b = t[:, :128], t[:, 128:]
        cos, sin = cos_s[s], sin_s[s]
        return jnp.concatenate([a * cos - b * sin, b * cos + a * sin], -1).astype(BF16)

    def turns():
        freq = freq_ref[...]

        def rows(i, _):
            s, n = i // 16, i % 16
            at = pl.ds(pl.multiple_of(16 * n, 16), 16)
            place = 256 * (r + 8 * s) + 16 * n + lax.broadcasted_iota(jnp.int32, (16, 128), 0)
            angle = place.astype(F32) * freq
            cos_s[s, at, :] = jnp.cos(angle)
            sin_s[s, at, :] = jnp.sin(angle)

        lax.fori_loop(0, 32, rows, None)

    def keys(s):
        a = a_s[s]
        k = _dot(a, wkv_s[0].reshape(2048, 256), 1, 0)
        v = _dot(a, wkv_s[1].reshape(2048, 256), 1, 0)
        kv_s[r + 8 * s, 0] = turn(k, s)
        kv_s[r + 8 * s, 1] = v.astype(BF16).T

    def queries(j):
        w = wq_s[j].reshape(2048, 512)
        for s in range(2):
            t = _dot(a_s[s], w, 1, 0)
            for h in range(2):
                q_s[s, 2 * j + h] = turn(t[:, 256 * h : 256 * h + 256], s)

    e = HEAD**-0.5 * LOG2E

    def unit(i, b, masked):
        k = kv_s[pl.ds(b, 2), 0].reshape(512, 256)
        ones = jnp.ones((8, 256), BF16)
        vt = jnp.concatenate([jnp.concatenate([kv_s[b + n, 1], ones], axis=0) for n in range(2)], axis=1)
        at = [slice(n, n + STRIP) for n in range(0, 2048, STRIP)]
        scores = [_dot(k, q_s[i, 2 * n : 2 * n + 2].reshape(STRIP, 256), 1, 1) for n in range(4)]
        if masked:
            gap = lax.broadcasted_iota(jnp.int32, (512, STRIP), 1) % 256 - lax.broadcasted_iota(jnp.int32, (512, STRIP), 0)
            scores = [jnp.where(gap >= -256 * c, s, HIDDEN) for s in scores]
        weights, keeps = [], []
        for n, s in enumerate(scores):
            old = top_s[i, :, at[n]]
            top = jnp.maximum(old, s.max(axis=0, keepdims=True))
            top_s[i, :, at[n]] = top
            weights.append(jnp.exp2((s - top) * e).astype(BF16))
            keeps.append(jnp.exp2((old - top) * e))
        for n in range(4):
            mix_s[i, :, at[n]] = mix_s[i, :, at[n]] * keeps[n] + _dot(vt, weights[n], 1, 0)

    def pair(i):
        return 4 * ((y + i // 2) % 2) + 2 * ((z + i % 2) % 2)

    def finish(i):
        for h in range(8):
            at = slice(256 * h, 256 * h + 256)
            seen_s[i, :, at] = (mix_s[i, :256, at] * (1 / mix_s[i, 256:257, at])).astype(BF16).T

    def share(j, s):
        return _dot(seen_s[s], wo_s[j].reshape(2048, 256), 1, 0)

    def project(j):
        w = wo_s[j].reshape(2048, 256)
        part_s[j] = _dot(seen_s[other], w, 1, 0).astype(BF16)
        own_s[j] = _dot(seen_s[x], w, 1, 0)

    def collect(j):
        swap_out(j).wait_recv()
        at = columns(256 * j, 256)
        y_ref[:, at] = (xs[x, :, at].astype(F32) + own_s[j] + got_s[j].astype(F32)).astype(BF16)

    barrier = pltpu.get_barrier_semaphore()
    for dev in (xdev, ydev, zdev, cdev):
        pl.semaphore_signal(barrier, inc=1, device_id={"sp": dev}, device_id_type=MESH)
    for copy in own_wk + own_wo[:1] + [own_x] + own_wq + own_wo[1:]:
        copy.start()
    pl.semaphore_wait(barrier, 4)
    swap_wk(0, wk_ref).start()
    swap_wk(1, wv_ref).start()
    for j in range(NQ):
        swap_wq(j).start()
    swap_x.start()

    def own_q(j):
        swap_wq(j).wait_recv()
        own(wq(j))

    whole_wk.wait()
    own(wka)
    own_wo[0].wait()
    own(wo(0))
    own_x.wait()
    norm(x)
    forward(wka)
    all_wk.wait_recv()
    own(wkb)
    forward(wo(0))
    whole_wq.wait()
    own_q(0)
    diagonal(wka)
    forward(wkb)
    own_q(1)
    turns()
    diagonal(wo(0))
    forward(wq(0))
    own_q(2)
    diagonal(wkb)
    complete(wka)
    complete(wkb)
    keys(x)
    forward(wq(1))
    own_q(3)
    diagonal(wq(0))
    forward(wq(2))
    diagonal(wq(1))
    swap_x.wait_recv()
    norm(other)
    forward(wq(3))
    own(kvo)
    keys(other)
    rest_wo.wait()
    own(kvp)

    def ask(j, _):
        @pl.when(j >= 2)
        def _():
            diagonal(wq(j))

        complete(wq(j))
        queries(j)

    lax.fori_loop(0, NQ, ask, None)

    top_s[...] = jnp.full(top_s.shape, NEG, F32)
    mix_s[...] = jnp.zeros(mix_s.shape, F32)
    onward(kvo)
    arrived(kvo, 1)
    arrived(kvp, 1)
    lax.fori_loop(0, 2, lambda i, _: unit(i, r - c + 8 * i, True), None)
    onward(kvp)
    own(wo(1))
    across(kvo)

    def attend(n, _):
        i = n // 3
        u = lax.select(n < 9, n % 3, (2 * (n - 9) + x) % 3)
        b = pair(i)

        def at(when, *what):
            @pl.when(n == when)
            def _():
                for f, part in what:
                    f(part)

        at(3, (across, kvp), (own, wo(2)))
        at(6, (onward, wo(1)), (own, wo(3)), (diagonal, kvo))
        at(8, (diagonal, kvp), (onward, wo(2)))
        at(9, (own, wo(4)), (across, wo(1)))
        at(10, (onward, wo(3)), (diagonal, wo(1)))
        at(11, (across, wo(2)), (own, wo(5)))

        @pl.when((n % 3 == 0) & (n > 0))
        def _():
            arrived(kvo, 2 * i + 1)
            arrived(kvp, 2 * i + 1)

        @pl.when(n == 11 - x)
        def _():
            finish(other)
            complete(wo(0))
            part_s[0] = share(0, other).astype(BF16)

        @pl.when((u == 0) | ((i > 0) & (b < r - c)))
        def _():
            unit((u + 1) % 2, b + 8 * (u // 2), False)

        @pl.when(n == 11 - x)
        def _():
            swap_out(0).start()

    lax.fori_loop(0, 12, attend, None)
    onward(wo(4))
    diagonal(wo(2))
    across(wo(3))
    finish(x)
    own_s[0] = share(0, x)

    def output(j, _):
        @pl.when(j > 2)
        def _():
            diagonal(wo(j))

        complete(wo(j))
        project(j)
        swap_out(j).start()

        @pl.when(j == 1)
        def _():
            own(wo(6))
            onward(wo(5))

        @pl.when(j == 2)
        def _():
            own(wo(7))
            across(wo(4))

        @pl.when(j == 3)
        def _():
            onward(wo(6))
            across(wo(5))

        @pl.when(j == 4)
        def _():
            onward(wo(7))
            across(wo(6))

        @pl.when(j == 5)
        def _():
            across(wo(7))

        @pl.when(j > 2)
        def _():
            collect(j - 3)

    lax.fori_loop(1, NO, output, None)
    for j in (NO - 3, NO - 2, NO - 1):
        collect(j)
    all_wk.wait_send()
    all_wq.wait_send()
    swap_x.wait_send()
    all_out.wait_send()
    for kind, what in ((0, wkv_s.at[:, pl.ds(0, 7)]), (1, wq_s.at[:, pl.ds(0, 7)]), (2, kv_s.at[pl.ds(0, 8)]), (3, wo_s.at[:, pl.ds(0, 7)])):
        remote(what, what, ss.at[kind], rs.at[0], cdev).wait_send()
    more = sum(flag.astype(jnp.int32) for flag in (to_y, to_z, to_far, to_core, from_second, y == 1))
    lax.fori_loop(0, more, lambda i, _: remote(kv_s.at[0], kv_s.at[0], ss.at[2], rs.at[0], cdev).wait_send(), None)


def solution(mesh):
    def step(x, gain, wq, wk, wv, wo):
        half = HEAD // 2
        freq = np.float32(THETA) ** (-np.arange(half, dtype=np.float32) / np.float32(half))
        anywhere, vmem = pl.BlockSpec(memory_space=pl.ANY), pl.BlockSpec(memory_space=pltpu.VMEM)
        return pl.pallas_call(
            kernel,
            out_shape=pltpu.VMEM((256, 2048), BF16),
            in_specs=[anywhere, vmem, vmem, anywhere, anywhere, anywhere, anywhere],
            out_specs=vmem,
            scratch_shapes=[
                pltpu.VMEM((2, 256, 2048), BF16),
                pltpu.VMEM((2, 256, 2048), BF16),
                pltpu.VMEM((2, 256, 128), F32),
                pltpu.VMEM((2, 256, 128), F32),
                pltpu.VMEM((2, 8, 256, 256), BF16),
                pltpu.VMEM((NQ, 8, 256, 512), BF16),
                pltpu.VMEM((NO, 8, 256, 256), BF16),
                pltpu.VMEM((16, 2, 256, 256), BF16),
                pltpu.VMEM((2, 8, 256, 256), BF16),
                pltpu.VMEM((2, 1, 2048), F32),
                pltpu.VMEM((2, 264, 2048), F32),
                pltpu.VMEM((2, 256, 2048), BF16),
                pltpu.VMEM((NO, 256, 256), BF16),
                pltpu.VMEM((NO, 256, 256), BF16),
                pltpu.VMEM((NO, 256, 256), F32),
                pltpu.SemaphoreType.DMA((4,)),
                pltpu.SemaphoreType.DMA((4 * PARTS + 8,)),
                pltpu.SemaphoreType.DMA((4,)),
                pltpu.SemaphoreType.DMA((2 + NQ + NO,)),
                pltpu.SemaphoreType.DMA((5,)),
            ],
            compiler_params=pltpu.CompilerParams(collective_id=0, has_side_effects=True, vmem_limit_bytes=58 * 2**20),
        )(x, gain, jnp.asarray(freq.astype(np.float32)).reshape(1, half), wq, wk, wv, wo)

    tokens, whole = P(("dp", "sp"), None), P("sp", None)
    return jax.shard_map(
        step,
        mesh=mesh,
        in_specs=(tokens, P(None), whole, whole, whole, whole),
        out_specs=tokens,
        check_vma=False,
    )
```

```python
import functools

import jax
import jax.numpy as jnp
import numpy as np
from jax import lax
from jax.experimental import pallas as pl
from jax.experimental.pallas import tpu as pltpu
from jax.sharding import PartitionSpec as P

HEAD = 256
THETA = 10000
NEG = -1e30
HIDDEN = 2 * NEG
LOG2E = 1.4426950408889634
MESH = pl.DeviceIdType.MESH
BF16, F32 = jnp.bfloat16, jnp.float32
STRIP = 512
NQ, NO = 4, 8
WKV, WQ, KVO, KVP, WO = 0, 2, 2 + NQ, 3 + NQ, 4 + NQ
PARTS = 4 + NQ + NO


def _dot(a, b, ca, cb):
    return lax.dot_general(a, b, (((ca,), (cb,)), ((), ())), preferred_element_type=F32)


def kernel(x_ref, gain_ref, freq_ref, wq_ref, wk_ref, wv_ref, wo_ref, y_ref,
           xs, a_s, cos_s, sin_s, wkv_s, wq_s, wo_s, kv_s, q_s, top_s, mix_s, seen_s, part_s, got_s, own_s,
           ss, rs, xss, xrs, ls):
    me = lax.axis_index("sp")
    x, y, z, c = me // 8, (me // 4) % 2, (me // 2) % 2, me % 2
    r = me % 8
    other = 1 - x
    xdev, ydev, zdev, cdev = me + 8 - 16 * x, me + 4 - 8 * y, me + 2 - 4 * z, me + 1 - 2 * c

    def rel(k):
        return 4 * ((y + k // 4) % 2) + 2 * ((z + (k // 2) % 2) % 2) + (c + k % 2) % 2

    first, second = 4 - 2 * c, 2 + 2 * c
    far = me + 2 - 4 * z + c * (4 - 8 * y - 2 + 4 * z)

    def remote(src, dst, ssem, rsem, dev):
        return pltpu.make_async_remote_copy(src_ref=src, dst_ref=dst, send_sem=ssem, recv_sem=rsem,
                                            device_id={"sp": dev}, device_id_type=MESH)

    def direct(part, slot):
        return rs.at[4 * part[1] + 4 - slot // 2]

    def passed(part, slot):
        return rs.at[4 * PARTS + 4 * (part[1] - KVO) + slot // 2] if part[2] == 2 else rs.at[4 * part[1]]

    def hop(part, src, sem, dev):
        return remote(part[0](src), part[0](src), ss.at[part[2]], sem, dev)

    def upward(part, need):
        return pl.when((part[3] == 0) | need) if part[2] == 2 else lambda f: f()

    early, late = c == 0, c == 1
    from_first = (early & (y == 1)) | (late & ((z == 1) | (y == 0)))
    to_core = (early & (y == 1)) | (late & (z == 1))
    from_second = (early & (z == 1)) | (late & (y == 1))
    to_far = (early & (y == 1)) | (late & (y == 0))
    to_y, to_z = y == 0, (z == 0) | (late & (y == 0))

    def own(part):
        @upward(part, to_y)
        def _():
            hop(part, r, direct(part, 4), ydev).start()

        @upward(part, to_z)
        def _():
            hop(part, r, direct(part, 2), zdev).start()

        hop(part, r, passed(part, 1), cdev).start()

    def onward(part):
        @upward(part, from_first)
        def _():
            hop(part, rel(first), direct(part, first), cdev).wait_recv()

        @upward(part, to_far)
        def _():
            hop(part, rel(first), direct(part, 6), far).start()

        @upward(part, to_core)
        def _():
            hop(part, rel(first), passed(part, first + 1), cdev).start()

    def across(part):
        @upward(part, from_second)
        def _():
            hop(part, rel(second), direct(part, second), cdev).wait_recv()
            hop(part, rel(second), passed(part, second + 1), cdev).start()

    def forward(part):
        onward(part)
        across(part)

    def diagonal(part):
        @upward(part, y == 1)
        def _():
            hop(part, rel(6), direct(part, 6), cdev).wait_recv()
            hop(part, rel(6), passed(part, 7), cdev).start()

    def complete(part):
        hop(part, pl.ds(0, 4), passed(part, 1), cdev).wait_recv()

    def arrived(part, slot):
        @upward(part, (slot == 1) | ((slot == 3) & (z == 1)) | ((slot > 3) & (y == 1)))
        def _():
            hop(part, rel(slot), passed(part, slot), cdev).wait_recv()

    mine = pl.ds(pl.multiple_of(128 * x, 128), 128)
    theirs = pl.ds(pl.multiple_of(128 * other, 128), 128)
    wka = (lambda s: wkv_s.at[:, s, mine], WKV, 0)
    wkb = (lambda s: wkv_s.at[:, s, theirs], WKV + 1, 0)
    kvo = (lambda s: kv_s.at[s + 8 * x], KVO, 2, x)
    kvp = (lambda s: kv_s.at[s + 8 * other], KVP, 2, other)

    def wq(j):
        return (lambda s: wq_s.at[j, s], WQ + j, 1)

    def wo(j):
        return (lambda s: wo_s.at[j, s], WO + j, 3)

    def columns(h, width):
        return pl.ds(pl.multiple_of(h, width), width)

    def swap_wk(i, ref):
        return remote(ref.at[:, columns(other * 256, 256)], wkv_s.at[i, r, mine], xss.at[0], xrs.at[0], xdev)

    def swap_wq(j):
        return remote(wq_ref.at[:, columns(other * 2048 + 512 * j, 512)], wq_s.at[j, r, mine], xss.at[1], xrs.at[2 + j], xdev)

    swap_x = remote(x_ref, xs.at[x], xss.at[2], xrs.at[1], xdev)

    def swap_out(j):
        return remote(part_s.at[j], got_s.at[j], xss.at[3], xrs.at[2 + NQ + j], xdev)

    all_wk = remote(wkv_s.at[:, r, theirs], wkv_s.at[:, r, theirs], xss.at[0], xrs.at[0], xdev)
    all_wq = remote(wq_s.at[:, r, theirs], wq_s.at[:, r, theirs], xss.at[1], xrs.at[2], xdev)
    all_out = remote(part_s, got_s, xss.at[3], xrs.at[2], xdev)

    def local(i, src, dst):
        return pltpu.make_async_copy(src, dst, ls.at[i])

    own_wk = [local(0, ref.at[:, columns(x * 256, 256)], wkv_s.at[i, r, mine]) for i, ref in ((0, wk_ref), (1, wv_ref))]
    own_wq = [local(1, wq_ref.at[:, columns(x * 2048 + 512 * j, 512)], wq_s.at[j, r, mine]) for j in range(NQ)]
    own_x = local(2, x_ref, xs.at[x])
    own_wo = [local(3 + (j > 0), wo_ref.at[:, pl.ds(256 * j, 256)], wo_s.at[j, r]) for j in range(NO)]
    whole_wk = local(0, wkv_s.at[:, r, mine], wkv_s.at[:, r, mine])
    whole_wq = local(1, wq_s.at[:, r, mine], wq_s.at[:, r, mine])
    rest_wo = local(4, wo_s.at[pl.ds(1, NO - 1), r], wo_s.at[pl.ds(1, NO - 1), r])

    def norm(s):
        def rows(i, _):
            at = pl.ds(pl.multiple_of(16 * i, 16), 16)
            wide = xs[s, at, :].astype(F32)
            scale = lax.rsqrt(jnp.mean(wide * wide, -1, keepdims=True) + 1e-6)
            a = (wide * scale * gain_ref[...].astype(F32).reshape(1, 2048)).astype(BF16)
            for b in range(16):
                to = 2 * (b % 8) + b // 8
                a_s[s, at, to * 128 : to * 128 + 128] = a[:, b * 128 : b * 128 + 128]

        lax.fori_loop(0, 16, rows, None)

    def turn(t, s):
        t = t.astype(BF16).astype(F32)
        a, b = t[:, :128], t[:, 128:]
        cos, sin = cos_s[s], sin_s[s]
        return jnp.concatenate([a * cos - b * sin, b * cos + a * sin], -1).astype(BF16)

    def turns():
        freq = freq_ref[...]

        def rows(i, _):
            s, n = i // 16, i % 16
            at = pl.ds(pl.multiple_of(16 * n, 16), 16)
            place = 256 * (r + 8 * s) + 16 * n + lax.broadcasted_iota(jnp.int32, (16, 128), 0)
            angle = place.astype(F32) * freq
            cos_s[s, at, :] = jnp.cos(angle)
            sin_s[s, at, :] = jnp.sin(angle)

        lax.fori_loop(0, 32, rows, None)

    def keys(s):
        a = a_s[s]
        k = _dot(a, wkv_s[0].reshape(2048, 256), 1, 0)
        v = _dot(a, wkv_s[1].reshape(2048, 256), 1, 0)
        kv_s[r + 8 * s, 0] = turn(k, s)
        kv_s[r + 8 * s, 1] = v.astype(BF16).T

    def queries(j):
        w = wq_s[j].reshape(2048, 512)
        for s in range(2):
            t = _dot(a_s[s], w, 1, 0)
            for h in range(2):
                q_s[s, 2 * j + h] = turn(t[:, 256 * h : 256 * h + 256], s)

    e = HEAD**-0.5 * LOG2E

    def unit(i, b, masked):
        k = kv_s[pl.ds(b, 2), 0].reshape(512, 256)
        ones = jnp.ones((8, 256), BF16)
        vt = jnp.concatenate([jnp.concatenate([kv_s[b + n, 1], ones], axis=0) for n in range(2)], axis=1)
        at = [slice(n, n + STRIP) for n in range(0, 2048, STRIP)]
        scores = [_dot(k, q_s[i, 2 * n : 2 * n + 2].reshape(STRIP, 256), 1, 1) for n in range(4)]
        if masked:
            gap = lax.broadcasted_iota(jnp.int32, (512, STRIP), 1) % 256 - lax.broadcasted_iota(jnp.int32, (512, STRIP), 0)
            scores = [jnp.where(gap >= -256 * c, s, HIDDEN) for s in scores]
        weights, keeps = [], []
        for n, s in enumerate(scores):
            old = top_s[i, :, at[n]]
            top = jnp.maximum(old, s.max(axis=0, keepdims=True))
            top_s[i, :, at[n]] = top
            weights.append(jnp.exp2((s - top) * e).astype(BF16))
            keeps.append(jnp.exp2((old - top) * e))
        for n in range(4):
            mix_s[i, :, at[n]] = mix_s[i, :, at[n]] * keeps[n] + _dot(vt, weights[n], 1, 0)

    def pair(i):
        return 4 * ((y + i // 2) % 2) + 2 * ((z + i % 2) % 2)

    def finish(i):
        for h in range(8):
            at = slice(256 * h, 256 * h + 256)
            seen_s[i, :, at] = (mix_s[i, :256, at] * (1 / mix_s[i, 256:257, at])).astype(BF16).T

    def share(j, s):
        return _dot(seen_s[s], wo_s[j].reshape(2048, 256), 1, 0)

    def project(j):
        w = wo_s[j].reshape(2048, 256)
        part_s[j] = _dot(seen_s[other], w, 1, 0).astype(BF16)
        own_s[j] = _dot(seen_s[x], w, 1, 0)

    def collect(j):
        swap_out(j).wait_recv()
        at = columns(256 * j, 256)
        y_ref[:, at] = (xs[x, :, at].astype(F32) + own_s[j] + got_s[j].astype(F32)).astype(BF16)

    barrier = pltpu.get_barrier_semaphore()
    for dev in (xdev, ydev, zdev, cdev):
        pl.semaphore_signal(barrier, inc=1, device_id={"sp": dev}, device_id_type=MESH)
    for copy in own_wk + own_wo[:1]:
        copy.start()
    pl.semaphore_wait(barrier, 4)
    swap_wk(0, wk_ref).start()
    swap_wk(1, wv_ref).start()
    for j in range(NQ):
        swap_wq(j).start()
    swap_x.start()

    def own_q(j):
        swap_wq(j).wait_recv()
        own(wq(j))

    whole_wk.wait()
    own(wka)
    own_wo[0].wait()
    own(wo(0))
    for copy in [own_x] + own_wq + own_wo[1:]:
        copy.start()
    own_x.wait()
    norm(x)
    forward(wka)
    all_wk.wait_recv()
    own(wkb)
    forward(wo(0))
    whole_wq.wait()
    own_q(0)
    diagonal(wka)
    forward(wkb)
    own_q(1)
    turns()
    diagonal(wo(0))
    forward(wq(0))
    own_q(2)
    diagonal(wkb)
    complete(wka)
    complete(wkb)
    keys(x)
    forward(wq(1))
    own_q(3)
    diagonal(wq(0))
    forward(wq(2))
    diagonal(wq(1))
    swap_x.wait_recv()
    norm(other)
    forward(wq(3))
    own(kvo)
    keys(other)
    rest_wo.wait()
    own(kvp)

    def ask(j, _):
        @pl.when(j >= 2)
        def _():
            diagonal(wq(j))

        complete(wq(j))
        queries(j)

    lax.fori_loop(0, NQ, ask, None)

    top_s[...] = jnp.full(top_s.shape, NEG, F32)
    mix_s[...] = jnp.zeros(mix_s.shape, F32)
    onward(kvo)
    arrived(kvo, 1)
    arrived(kvp, 1)
    lax.fori_loop(0, 2, lambda i, _: unit(i, r - c + 8 * i, True), None)
    onward(kvp)
    own(wo(1))
    across(kvo)

    def attend(n, _):
        i = n // 3
        u = lax.select(n < 9, n % 3, (2 * (n - 9) + x) % 3)
        b = pair(i)

        def at(when, *what):
            @pl.when(n == when)
            def _():
                for f, part in what:
                    f(part)

        at(3, (across, kvp), (own, wo(2)))
        at(6, (onward, wo(1)), (own, wo(3)), (diagonal, kvo))
        at(8, (diagonal, kvp), (onward, wo(2)))
        at(9, (own, wo(4)), (across, wo(1)))
        at(10, (onward, wo(3)), (diagonal, wo(1)))
        at(11, (across, wo(2)), (own, wo(5)))

        @pl.when((n % 3 == 0) & (n > 0))
        def _():
            arrived(kvo, 2 * i + 1)
            arrived(kvp, 2 * i + 1)

        @pl.when(n == 11 - x)
        def _():
            finish(other)
            complete(wo(0))
            part_s[0] = share(0, other).astype(BF16)

        @pl.when((u == 0) | ((i > 0) & (b < r - c)))
        def _():
            unit((u + 1) % 2, b + 8 * (u // 2), False)

        @pl.when(n == 11 - x)
        def _():
            swap_out(0).start()

    lax.fori_loop(0, 12, attend, None)
    onward(wo(4))
    diagonal(wo(2))
    across(wo(3))
    finish(x)
    own_s[0] = share(0, x)

    def output(j, _):
        @pl.when(j > 2)
        def _():
            diagonal(wo(j))

        complete(wo(j))
        project(j)
        swap_out(j).start()

        @pl.when(j == 1)
        def _():
            own(wo(6))
            onward(wo(5))

        @pl.when(j == 2)
        def _():
            own(wo(7))
            across(wo(4))

        @pl.when(j == 3)
        def _():
            onward(wo(6))
            across(wo(5))

        @pl.when(j == 4)
        def _():
            onward(wo(7))
            across(wo(6))

        @pl.when(j == 5)
        def _():
            across(wo(7))

        @pl.when(j > 2)
        def _():
            collect(j - 3)

    lax.fori_loop(1, NO, output, None)
    for j in (NO - 3, NO - 2, NO - 1):
        collect(j)
    all_wk.wait_send()
    all_wq.wait_send()
    swap_x.wait_send()
    all_out.wait_send()
    for kind, what in ((0, wkv_s.at[:, pl.ds(0, 7)]), (1, wq_s.at[:, pl.ds(0, 7)]), (2, kv_s.at[pl.ds(0, 8)]), (3, wo_s.at[:, pl.ds(0, 7)])):
        remote(what, what, ss.at[kind], rs.at[0], cdev).wait_send()
    more = sum(flag.astype(jnp.int32) for flag in (to_y, to_z, to_far, to_core, from_second, y == 1))
    lax.fori_loop(0, more, lambda i, _: remote(kv_s.at[0], kv_s.at[0], ss.at[2], rs.at[0], cdev).wait_send(), None)


def solution(mesh):
    def step(x, gain, wq, wk, wv, wo):
        half = HEAD // 2
        freq = np.float32(THETA) ** (-np.arange(half, dtype=np.float32) / np.float32(half))
        anywhere, vmem = pl.BlockSpec(memory_space=pl.ANY), pl.BlockSpec(memory_space=pltpu.VMEM)
        return pl.pallas_call(
            kernel,
            out_shape=pltpu.VMEM((256, 2048), BF16),
            in_specs=[anywhere, vmem, vmem, anywhere, anywhere, anywhere, anywhere],
            out_specs=vmem,
            scratch_shapes=[
                pltpu.VMEM((2, 256, 2048), BF16),
                pltpu.VMEM((2, 256, 2048), BF16),
                pltpu.VMEM((2, 256, 128), F32),
                pltpu.VMEM((2, 256, 128), F32),
                pltpu.VMEM((2, 8, 256, 256), BF16),
                pltpu.VMEM((NQ, 8, 256, 512), BF16),
                pltpu.VMEM((NO, 8, 256, 256), BF16),
                pltpu.VMEM((16, 2, 256, 256), BF16),
                pltpu.VMEM((2, 8, 256, 256), BF16),
                pltpu.VMEM((2, 1, 2048), F32),
                pltpu.VMEM((2, 264, 2048), F32),
                pltpu.VMEM((2, 256, 2048), BF16),
                pltpu.VMEM((NO, 256, 256), BF16),
                pltpu.VMEM((NO, 256, 256), BF16),
                pltpu.VMEM((NO, 256, 256), F32),
                pltpu.SemaphoreType.DMA((4,)),
                pltpu.SemaphoreType.DMA((4 * PARTS + 8,)),
                pltpu.SemaphoreType.DMA((4,)),
                pltpu.SemaphoreType.DMA((2 + NQ + NO,)),
                pltpu.SemaphoreType.DMA((5,)),
            ],
            compiler_params=pltpu.CompilerParams(collective_id=0, has_side_effects=True, vmem_limit_bytes=58 * 2**20),
        )(x, gain, jnp.asarray(freq.astype(np.float32)).reshape(1, half), wq, wk, wv, wo)

    tokens, whole = P(("dp", "sp"), None), P("sp", None)
    return jax.shard_map(
        step,
        mesh=mesh,
        in_specs=(tokens, P(None), whole, whole, whole, whole),
        out_specs=tokens,
        check_vma=False,
    )
```
